16 devices in a mesh: dp: 2 (over y, z), tp: 8 (over x, core).
Axes of the slice: x: 4, y: 2, z: 1, core: 2. Of those that a mesh axis runs over, the one named last changes fastest.
The devices are a block of a 4x4x8 slice.
Arguments:
- hidden: bfloat16 [4, 2048, 2048], P('dp'), parts along dimension 0
- lengths: int32 [4], P('dp'), parts along dimension 0
- w_query: bfloat16 [2, 2048, 8, 256], P(None, None, 'tp')
- w_key: bfloat16 [2, 2048, 8, 256], P(None, None, 'tp')
- w_value: bfloat16 [2, 2048, 8, 256], P(None, None, 'tp')
- w_out: bfloat16 [2, 8, 256, 2048], P(None, 'tp')
- w_gate: bfloat16 [2, 2048, 8192], P(None, None, 'tp')
- w_up: bfloat16 [2, 2048, 8192], P(None, None, 'tp')
- w_down: bfloat16 [2, 8192, 2048], P(None, 'tp')
- norm_attn: float32 [2, 2048], replicated
- norm_mlp: float32 [2, 2048], replicated
Outputs:
- output 1: bfloat16 [4, 2048, 2048], P('dp'), parts along dimension 0
- output 2: bfloat16 [2, 4, 8, 2048, 256], P(None, 'dp', 'tp'), parts along dimension 1
- output 3: bfloat16 [2, 4, 8, 2048, 256], P(None, 'dp', 'tp'), parts along dimension 1
There are 2 independent parts. The reference program is written for one: setup_inputs(seed, part) draws one part's arguments, and reference() takes and returns one part's arrays. A program takes and returns all parts, laid end to end along the dimension named above; an argument that names none is the same for every part.
All inputs are finite; a program needn't handle non-finite values.
Results may differ from the reference program's by a relative error of at most 0.018677.
Values are sent between devices in bfloat16 or wider.
A program may use at most 768 MiB of HBM per device.

```python
import jax
import jax.numpy as jnp
from jax import lax

BATCH_ROWS = 2
SEQ_LEN = 2048
D_MODEL = 2048
N_HEADS = 8
HEAD_DIM = 256
FF_DIM = 8192
LAYER_COUNT = 2
INNER_DIM = N_HEADS * HEAD_DIM
RMS_EPS = 1e-6
ROPE_BASE = 10000.0


def draw_lengths(len_key):
    key_len, key_full = jax.random.split(len_key)
    drawn = jax.random.randint(key_len, (BATCH_ROWS,), 1, SEQ_LEN + 1)
    full_row = jax.random.randint(key_full, (), 0, BATCH_ROWS)
    return jnp.where(jnp.arange(BATCH_ROWS) == full_row, SEQ_LEN, drawn).astype(jnp.int32)


def setup_inputs(seed: int = 0, part: int = 0) -> dict:
    base_key = jax.random.key(seed)
    part_key = jax.random.fold_in(base_key, part)
    hid_key, len_key = jax.random.split(part_key)
    weight_keys = jax.random.split(base_key, 9)

    def normal_bf16(draw_key, shape, fan_in):
        return (jax.random.normal(draw_key, shape, jnp.float32) * fan_in ** -0.5).astype(jnp.bfloat16)

    qkv_shape = (LAYER_COUNT, D_MODEL, N_HEADS, HEAD_DIM)
    return {
        "hidden": jax.random.normal(hid_key, (BATCH_ROWS, SEQ_LEN, D_MODEL), jnp.float32).astype(jnp.bfloat16),
        "lengths": draw_lengths(len_key),
        "w_query": normal_bf16(weight_keys[0], qkv_shape, D_MODEL),
        "w_key": normal_bf16(weight_keys[1], qkv_shape, D_MODEL),
        "w_value": normal_bf16(weight_keys[2], qkv_shape, D_MODEL),
        "w_out": normal_bf16(weight_keys[3], (LAYER_COUNT, N_HEADS, HEAD_DIM, D_MODEL), INNER_DIM),
        "w_gate": normal_bf16(weight_keys[4], (LAYER_COUNT, D_MODEL, FF_DIM), D_MODEL),
        "w_up": normal_bf16(weight_keys[5], (LAYER_COUNT, D_MODEL, FF_DIM), D_MODEL),
        "w_down": normal_bf16(weight_keys[6], (LAYER_COUNT, FF_DIM, D_MODEL), FF_DIM),
        "norm_attn": 0.3 * jax.random.normal(weight_keys[7], (LAYER_COUNT, D_MODEL), jnp.float32),
        "norm_mlp": 0.3 * jax.random.normal(weight_keys[8], (LAYER_COUNT, D_MODEL), jnp.float32),
    }


def rms_norm(x_in, norm_gain):
    x_f32 = x_in.astype(jnp.float32)
    mean_sq = jnp.mean(x_f32 * x_f32, axis=-1, keepdims=True)
    return (x_f32 * lax.rsqrt(mean_sq + RMS_EPS) * (1.0 + norm_gain)).astype(jnp.bfloat16)


def apply_rope(x_in, cos_t, sin_t):
    half_dim = HEAD_DIM // 2
    x_low = x_in[..., :half_dim]
    x_high = x_in[..., half_dim:]
    return jnp.concatenate([x_low * cos_t - x_high * sin_t, x_high * cos_t + x_low * sin_t], axis=-1)


def one_layer(x_in, params, length, cos_t, sin_t):
    w_query, w_key, w_value, w_out, w_gate, w_up, w_down, gain_attn, gain_mlp = params
    normed = rms_norm(x_in, gain_attn)
    query = jnp.dot(normed, w_query.reshape(D_MODEL, INNER_DIM), preferred_element_type=jnp.float32).reshape(SEQ_LEN, N_HEADS, HEAD_DIM)
    keys = jnp.dot(normed, w_key.reshape(D_MODEL, INNER_DIM), preferred_element_type=jnp.float32).reshape(SEQ_LEN, N_HEADS, HEAD_DIM)
    values = jnp.dot(normed, w_value.reshape(D_MODEL, INNER_DIM), preferred_element_type=jnp.float32).astype(jnp.bfloat16).reshape(SEQ_LEN, N_HEADS, HEAD_DIM)
    query_rot = (apply_rope(query, cos_t, sin_t) * HEAD_DIM ** -0.5).astype(jnp.bfloat16)
    key_rot = apply_rope(keys, cos_t, sin_t).astype(jnp.bfloat16)
    scores = jnp.einsum("qhd,khd->hqk", query_rot.astype(jnp.float32), key_rot.astype(jnp.float32))
    positions = jnp.arange(SEQ_LEN)
    allowed = (positions[None, :] <= positions[:, None]) & (positions[None, :] < length)
    scores = jnp.where(allowed[None, :, :], scores, -1e30)
    attn_probs = jax.nn.softmax(scores, axis=-1).astype(jnp.bfloat16)
    attn_out = jnp.einsum("hqk,khd->qhd", attn_probs.astype(jnp.float32), values.astype(jnp.float32)).astype(jnp.bfloat16)
    attn_proj = jnp.dot(attn_out.reshape(SEQ_LEN, INNER_DIM), w_out.reshape(INNER_DIM, D_MODEL), preferred_element_type=jnp.float32)
    mid_state = (x_in.astype(jnp.float32) + attn_proj).astype(jnp.bfloat16)
    normed_mlp = rms_norm(mid_state, gain_mlp)
    gate_pre = jnp.dot(normed_mlp, w_gate, preferred_element_type=jnp.float32)
    up_proj = jnp.dot(normed_mlp, w_up, preferred_element_type=jnp.float32)
    hidden_act = (jax.nn.gelu(gate_pre, approximate=True) * up_proj).astype(jnp.bfloat16)
    down_proj = jnp.dot(hidden_act, w_down, preferred_element_type=jnp.float32)
    out_state = (mid_state.astype(jnp.float32) + down_proj).astype(jnp.bfloat16)
    return out_state, (jnp.swapaxes(key_rot, 0, 1), jnp.swapaxes(values, 0, 1))


def reference(hidden, lengths, w_query, w_key, w_value, w_out, w_gate, w_up, w_down, norm_attn, norm_mlp):
    inv_freq = ROPE_BASE ** (-jnp.arange(HEAD_DIM // 2, dtype=jnp.float32) * (2.0 / HEAD_DIM))
    angles = jnp.arange(SEQ_LEN, dtype=jnp.float32)[:, None] * inv_freq[None, :]
    cos_t = jnp.cos(angles)[:, None, :]
    sin_t = jnp.sin(angles)[:, None, :]
    stacked = (w_query, w_key, w_value, w_out, w_gate, w_up, w_down, norm_attn, norm_mlp)

    def one_row(row_args):
        row_hidden, row_length = row_args

        def layer_step(carry, params):
            return one_layer(carry, params, row_length, cos_t, sin_t)

        return lax.scan(layer_step, row_hidden, stacked)

    out_rows, caches = lax.map(one_row, (hidden, lengths))
    key_rows, value_rows = caches
    return out_rows, jnp.swapaxes(key_rows, 0, 1), jnp.swapaxes(value_rows, 0, 1)
```

```python
import functools

import jax
import jax.numpy as jnp
from jax import lax
from jax.experimental import pallas as pl
from jax.experimental.pallas import tpu as pltpu
from jax.sharding import Mesh
from jax.sharding import PartitionSpec as P

RMS_EPS = 1e-6
ROPE_BASE = 10000.0
CORES = 2
CHUNKS = 4
ROW_TILE = 256
FF_TILE = 512
VMEM = 56 * 1024 * 1024


def cost(flops, nbytes, exps=0):
    return pl.CostEstimate(flops=int(flops), bytes_accessed=int(nbytes), transcendentals=int(exps))


def params(**kw):
    return pltpu.CompilerParams(vmem_limit_bytes=VMEM, **kw)


def norm_rows(x_f32, gain):
    mean_sq = jnp.mean(x_f32 * x_f32, axis=-1, keepdims=True)
    return (x_f32 * lax.rsqrt(mean_sq + RMS_EPS) * (1.0 + gain)).astype(jnp.bfloat16)


def qkv_kernel(x_ref, gain_ref, cos_ref, sin_ref, *refs):
    w_refs, (q_ref, k_ref, v_ref) = refs[:-3], refs[-3:]
    normed = norm_rows(x_ref[...].astype(jnp.float32), gain_ref[...])
    cos_t, sin_t = cos_ref[...], sin_ref[...]
    half = cos_t.shape[-1]
    heads = len(w_refs) // 3

    def rope(y, scale):
        low, high = y[:, :half], y[:, half:]
        return jnp.concatenate([(low * cos_t - high * sin_t) * scale, (high * cos_t + low * sin_t) * scale], axis=-1)

    for j in range(heads):
        query = jnp.dot(normed, w_refs[j][...], preferred_element_type=jnp.float32)
        q_ref[j] = rope(query, (2 * half) ** -0.5).astype(jnp.bfloat16)
        keys = jnp.dot(normed, w_refs[heads + j][...], preferred_element_type=jnp.float32)
        k_ref[j] = rope(keys, 1.0).astype(jnp.bfloat16)
        v_ref[j] = jnp.dot(normed, w_refs[2 * heads + j][...], preferred_element_type=jnp.float32).astype(jnp.bfloat16)


def qkv_call(x, gain, cos_t, sin_t, weights):
    rows, width = x.shape
    head = weights[0].shape[-1]
    heads = len(weights) // 3
    tile = min(ROW_TILE, rows)
    out = jax.ShapeDtypeStruct((heads, rows, head), jnp.bfloat16)
    out_spec = pl.BlockSpec((heads, tile, head), lambda i: (0, i, 0))
    whole = pl.BlockSpec((width, head), lambda i: (0, 0), pipeline_mode=pl.Buffered(1))
    table = pl.BlockSpec((tile, head // 2), lambda i: (i, 0))
    return pl.pallas_call(
        qkv_kernel,
        grid=(rows // tile,),
        out_shape=(out, out, out),
        in_specs=[pl.BlockSpec((tile, width), lambda i: (i, 0)), pl.BlockSpec((1, width), lambda i: (0, 0)), table, table]
        + [whole] * len(weights),
        out_specs=(out_spec, out_spec, out_spec),
        compiler_params=params(),
        cost_estimate=cost(2 * rows * width * head * len(weights), 2 * len(weights) * width * head + 2 * rows * width),
    )(x, gain, cos_t, sin_t, *weights)


def attention_kernel(first, len_ref, q_ref, *refs):
    count = (len(refs) - 1) // 2
    k_refs, v_refs, o_ref = refs[:count], refs[count : 2 * count], refs[-1]
    rows = q_ref.shape[1]
    length = len_ref[0]
    query = q_ref[0]
    dims = (((1,), (1,)), ((), ()))
    row_id = lax.broadcasted_iota(jnp.int32, (rows, rows), 0)
    col_id = lax.broadcasted_iota(jnp.int32, (rows, rows), 1)
    blocks = []
    for j in range(count):
        scores = lax.dot_general(query, k_refs[j][0], dims, preferred_element_type=jnp.float32)
        allowed = col_id < length - j * rows
        if j == count - 1:
            allowed = allowed & (col_id <= row_id)
        blocks.append(jnp.where(allowed, scores, -1e30))
    top = functools.reduce(jnp.maximum, [jnp.max(b, axis=-1, keepdims=True) for b in blocks])
    blocks = [jnp.exp(b - top) for b in blocks]
    inv = 1.0 / functools.reduce(jnp.add, [jnp.sum(b, axis=-1, keepdims=True) for b in blocks])
    total = None
    for j in range(count):
        part = jnp.dot((blocks[j] * inv).astype(jnp.bfloat16), v_refs[j][0], preferred_element_type=jnp.float32)
        total = part if total is None else total + part
    o_ref[...] = total.astype(jnp.bfloat16)


def attention_call(length, query, k_list, v_list):
    heads, rows, head = query.shape
    count = len(k_list)
    spec = pl.BlockSpec((1, rows, head), lambda h: (h, 0, 0))
    return pl.pallas_call(
        functools.partial(attention_kernel, count),
        grid=(heads,),
        out_shape=jax.ShapeDtypeStruct((rows, heads * head), jnp.bfloat16),
        in_specs=[pl.BlockSpec(memory_space=pltpu.SMEM)] + [spec] * (1 + 2 * count),
        out_specs=pl.BlockSpec((rows, head), lambda h: (0, h)),
        compiler_params=params(),
        cost_estimate=cost(4 * heads * rows * rows * count * head * 2, 4 * heads * rows * count * head, heads * rows * rows * count),
    )(length, query, *k_list, *v_list)


def out_kernel(x_ref, o_ref, w_ref, gain_ref, mid_ref, normed_ref):
    total = x_ref[...].astype(jnp.float32)
    acc = None
    for c in range(o_ref.shape[0]):
        part = jnp.dot(o_ref[c], w_ref[c], preferred_element_type=jnp.float32)
        acc = part if acc is None else acc + part
    mid = (total + acc).astype(jnp.bfloat16)
    mid_ref[...] = mid
    normed_ref[...] = norm_rows(mid.astype(jnp.float32), gain_ref[...])


def out_call(x, o_all, w_out, gain):
    rows, width = x.shape
    chips, _, inner = o_all.shape
    tile = min(ROW_TILE, rows)
    row_spec = pl.BlockSpec((tile, width), lambda i: (i, 0))
    out = jax.ShapeDtypeStruct((rows, width), jnp.bfloat16)
    return pl.pallas_call(
        out_kernel,
        grid=(rows // tile,),
        out_shape=(out, out),
        in_specs=[
            row_spec,
            pl.BlockSpec((chips, tile, inner), lambda i: (0, i, 0)),
            pl.BlockSpec((chips, inner, width), lambda i: (0, 0, 0), pipeline_mode=pl.Buffered(1)),
            pl.BlockSpec((1, width), lambda i: (0, 0)),
        ],
        out_specs=(row_spec, row_spec),
        compiler_params=params(),
        cost_estimate=cost(2 * rows * chips * inner * width, 2 * chips * inner * width + 8 * rows * width),
    )(x, o_all, w_out, gain)


def mlp_kernel(a_ref, wg_m, wg_o, wu_m, wu_o, wd_m, wd_o, p_ref, acc_ref):
    step = pl.program_id(0)
    normed = a_ref[...]
    acc = None
    for wg, wu, wd in ((wg_m, wu_m, wd_m), (wg_o, wu_o, wd_o)):
        gate = jnp.dot(normed, wg[...], preferred_element_type=jnp.float32)
        up = jnp.dot(normed, wu[...], preferred_element_type=jnp.float32)
        act = (jax.nn.gelu(gate, approximate=True) * up).astype(jnp.bfloat16)
        part = jnp.dot(act, wd[...], preferred_element_type=jnp.float32)
        acc = part if acc is None else acc + part

    @pl.when(step == 0)
    def _():
        acc_ref[...] = acc

    @pl.when(step > 0)
    def _():
        acc_ref[...] += acc

    @pl.when(step == pl.num_programs(0) - 1)
    def _():
        p_ref[...] = acc_ref[...].astype(jnp.bfloat16)


def mlp_call(normed, gate, up, down, layer):
    rows, width = normed.shape
    ff = gate[0].shape[-1]
    tile = min(FF_TILE, ff)
    col = pl.BlockSpec((None, width, tile), lambda i: (layer, 0, i))
    col_p = pl.BlockSpec((width, tile), lambda i: (0, i))
    row = pl.BlockSpec((None, tile, width), lambda i: (layer, i, 0))
    row_p = pl.BlockSpec((tile, width), lambda i: (i, 0))
    return pl.pallas_call(
        mlp_kernel,
        grid=(ff // tile,),
        out_shape=jax.ShapeDtypeStruct((rows, width), jnp.bfloat16),
        in_specs=[pl.BlockSpec((rows, width), lambda i: (0, 0), pipeline_mode=pl.Buffered(1)), col, col_p, col, col_p, row, row_p],
        out_specs=pl.BlockSpec((rows, width), lambda i: (0, 0), pipeline_mode=pl.Buffered(1)),
        scratch_shapes=[pltpu.VMEM((rows, width), jnp.float32)],
        compiler_params=params(),
        cost_estimate=cost(12 * rows * width * ff, 12 * width * ff + 4 * rows * width, 2 * rows * ff),
    )(normed, gate[0], gate[1], up[0], up[1], down[0], down[1])


def rope_tables(seq_len, head_dim):
    half_dim = head_dim // 2
    inv_freq = ROPE_BASE ** (-jnp.arange(half_dim, dtype=jnp.float32) * (2.0 / head_dim))
    angles = jnp.arange(seq_len, dtype=jnp.float32)[:, None] * inv_freq[None, :]
    return jnp.cos(angles), jnp.sin(angles)


def solution(mesh):
    groups, members = mesh.devices.shape
    chips = members // CORES
    fine = Mesh(mesh.devices.reshape(groups, chips, CORES), ("dp", "x", "core"))
    tp = ("x", "core")
    swap = [(0, 1), (1, 0)]

    def partner(value):
        return lax.ppermute(value, "core", swap)

    def shard_body(hidden, lengths, w_query, w_key, w_value, w_out, w_gate, w_up, w_down, norm_attn, norm_mlp):
        core = lax.axis_index("core")
        chip = lax.axis_index("x")
        layers = w_query.shape[0]
        seq, width = hidden.shape[1:]
        head = w_query.shape[-1]
        rows = seq // CHUNKS
        part = rows // chips
        length = lax.dynamic_slice_in_dim(lengths, core, 1)
        x_full = lax.dynamic_index_in_dim(hidden, core, keepdims=False)
        x = [x_full[i * rows : (i + 1) * rows] for i in range(CHUNKS)]
        cos_t, sin_t = rope_tables(seq, head)
        wo_all = []
        qkv_w = []
        mlp_w = []
        for l in range(layers):
            own = [w[l].reshape(width, head) for w in (w_query, w_key, w_value)]
            other = [partner(w) for w in own]
            qkv_w.append([w for pair in zip(own, other) for w in pair])
        for l in range(layers):
            mlp_w.append([(w, partner(w[l])) for w in (w_gate, w_up, w_down)])
            own_rows = lax.all_gather(w_out[l].reshape(head, width), "x")
            wo_all.append(jnp.concatenate([own_rows, partner(own_rows)], axis=1))
        k_cache = []
        v_cache = []
        for l in range(layers):
            keys, values = [], []
            for i in range(CHUNKS):
                tables = (cos_t[i * rows : (i + 1) * rows], sin_t[i * rows : (i + 1) * rows])
                q, k, v = qkv_call(x[i], norm_attn[l][None, :], *tables, qkv_w[l])
                keys.append(k)
                values.append(v)
                o = attention_call(length, q, keys, values)
                o_all = lax.all_gather(o, "x")
                mid, normed = out_call(x[i], o_all, wo_all[l], norm_mlp[l][None, :])
                partial = mlp_call(normed, *mlp_w[l], l)
                summed = lax.psum_scatter(partial, "x", scatter_dimension=0, tiled=True)
                mine = lax.dynamic_slice_in_dim(mid, chip * part, part, axis=0)
                mine = (mine.astype(jnp.float32) + summed.astype(jnp.float32)).astype(jnp.bfloat16)
                if l < layers - 1:
                    x[i] = lax.all_gather(mine, "x", axis=0, tiled=True)
                else:
                    both = lax.all_gather(mine, tp).reshape(chips, CORES, part, width)
                    x[i] = jnp.swapaxes(both, 0, 1).reshape(CORES, rows, width)
            for cache, pieces in ((k_cache, keys), (v_cache, values)):
                own = jnp.concatenate([p[0] for p in pieces], axis=0)
                got = partner(jnp.concatenate([p[1] for p in pieces], axis=0))
                pair = jnp.where(core == 0, jnp.stack([own, got]), jnp.stack([got, own]))
                cache.append(pair[:, None])
        return jnp.concatenate(x, axis=1), jnp.stack(k_cache), jnp.stack(v_cache)

    head_cols = P(None, None, tp, None)
    return jax.shard_map(
        shard_body,
        mesh=fine,
        in_specs=(P("dp"), P("dp"), head_cols, head_cols, head_cols, P(None, tp, None, None), P(None, None, tp), P(None, None, tp), P(None, tp, None), P(), P()),
        out_specs=(P("dp"), P(None, "dp", tp), P(None, "dp", tp)),
        check_vma=False,
    )
```

```python
import functools

import jax
import jax.numpy as jnp
from jax import lax
from jax.experimental import pallas as pl
from jax.experimental.pallas import tpu as pltpu
from jax.sharding import Mesh
from jax.sharding import PartitionSpec as P


RMS_EPS = 1e-6
ROPE_BASE = 10000.0
CORES = 2
CHIPS = 4
CHUNKS = 4
ROW_TILE = 256
FF_TILE = 256
VMEM = 60 * 1024 * 1024
BF16 = jnp.bfloat16
F32 = jnp.float32
ANY = pl.BlockSpec(memory_space=pl.ANY)
SMEM = pl.BlockSpec(memory_space=pltpu.SMEM)
OFFSETS = (0, 3, 1, 2)


def cost(flops, nbytes, exps=0):
    return pl.CostEstimate(flops=int(flops), bytes_accessed=int(nbytes), transcendentals=int(exps))


def norm_rows(x_f32, gain):
    mean_sq = jnp.mean(x_f32 * x_f32, axis=-1, keepdims=True)
    return (x_f32 * lax.rsqrt(mean_sq + RMS_EPS) * (1.0 + gain)).astype(BF16)


def struct(shape, dtype=BF16):
    return jax.ShapeDtypeStruct(shape, dtype)


def whole(shape):
    return pl.BlockSpec(shape, lambda *_: (0,) * len(shape))


def piece_rows(ids_ref, place, half, part):
    return pl.multiple_of(lax.rem(ids_ref[0] + OFFSETS[place], CHIPS) * part + half * (part // 2), part // 2)


def front_kernel(layer, chunk, pieces, ids_ref, len_ref, gain_ref, cos_ref, sin_ref, *refs):
    refs = list(refs)
    x_refs = [refs.pop(0) for _ in range(8 if pieces else 1)]
    w_refs = [refs.pop(0) for _ in range(6)]
    old = [[refs.pop(0) for _ in range(chunk)] for _ in range(4)]
    x_out = refs.pop(0) if pieces else None
    new = [refs.pop(0) for _ in range(4)]
    o_refs = [refs.pop(0) for _ in range(2)]
    x_buf, normed, w_buf, q_buf, x_sem, w_sem, out_sem = refs
    rows, _ = x_buf.shape
    head = q_buf.shape[-1]
    half = head // 2
    if pieces:
        part = rows // CHIPS
        copies = [
            pltpu.make_async_copy(x_refs[n], x_buf.at[pl.ds(piece_rows(ids_ref, n // 2, n % 2, part), part // 2)], x_sem.at[n])
            for n in range(8)
        ]
    else:
        copies = [pltpu.make_async_copy(x_refs[0].at[ids_ref[1], pl.ds(chunk * rows, rows)], x_buf, x_sem.at[0])]
    for c in copies:
        c.start()
    loads = [pltpu.make_async_copy(w_refs[n].at[layer], w_buf.at[n], w_sem.at[n]) for n in range(6)]
    for c in loads:
        c.start()
    for c in copies:
        c.wait()
    save = None
    if pieces:
        save = pltpu.make_async_copy(x_buf, x_out, out_sem)
        save.start()
    tile = min(ROW_TILE, rows)
    for r in range(0, rows, tile):
        normed[pl.ds(r, tile)] = norm_rows(x_buf[pl.ds(r, tile)].astype(F32), gain_ref[...])

    def rope(y, at):
        low, high = y[:, :half], y[:, half:]
        c, s = cos_ref[pl.ds(at, tile)], sin_ref[pl.ds(at, tile)]
        return jnp.concatenate([low * c - high * s, high * c + low * s], axis=-1)

    for n in range(6):
        loads[n].wait()
        for r in range(0, rows, tile):
            y = jnp.dot(normed[pl.ds(r, tile)], w_buf[n], preferred_element_type=F32)
            if n < 2:
                q_buf[n, pl.ds(r, tile)] = (rope(y, r) * head**-0.5).astype(BF16)
            elif n < 4:
                new[n - 2][pl.ds(r, tile)] = rope(y, r).astype(BF16)
            else:
                new[n - 2][pl.ds(r, tile)] = y.astype(BF16)

    dims = (((1,), (1,)), ((), ()))
    length = len_ref[0]
    col = lax.broadcasted_iota(jnp.int32, (1, rows), 1)
    lower = lax.broadcasted_iota(jnp.int32, (tile, rows), 1) - lax.broadcasted_iota(jnp.int32, (tile, rows), 0)
    bias = [jnp.where(col < length - j * rows, 0.0, -1e30).astype(F32) for j in range(chunk + 1)]
    for h in range(2):
        keys = old[h] + [new[h]]
        values = old[2 + h] + [new[2 + h]]
        for r in range(0, rows, tile):
            query = q_buf[h, pl.ds(r, tile)]
            blocks = []
            for j in range(chunk + 1):
                scores = lax.dot_general(query, keys[j][...], dims, preferred_element_type=F32) + bias[j]
                if j == chunk:
                    scores = jnp.where(lower <= r, scores, -1e30)
                blocks.append(scores)
            top = functools.reduce(jnp.maximum, [jnp.max(b, axis=-1, keepdims=True) for b in blocks])
            blocks = [jnp.exp(b - top) for b in blocks]
            inv = 1.0 / functools.reduce(jnp.add, [jnp.sum(b, axis=-1, keepdims=True) for b in blocks])
            total = None
            for j in range(chunk + 1):
                prod = jnp.dot((blocks[j] * inv).astype(BF16), values[j][...], preferred_element_type=F32)
                total = prod if total is None else total + prod
            o_refs[h][pl.ds(r, tile)] = total.astype(BF16)
    if save is not None:
        save.wait()


def front_call(layer, chunk, ids, length, gain, cos_t, sin_t, x_list, weights, old, rows):
    width, head = weights[0].shape[1:]
    pieces = len(x_list) > 1
    small = whole((rows, head))
    table = pl.BlockSpec((rows, head // 2), lambda *_: (chunk, 0))
    flops = 12 * rows * width * head + 8 * rows * rows * (chunk + 1) * head
    out_shape = [struct((rows, head))] * 6
    out_specs = [small] * 6
    if pieces:
        out_shape = [struct((rows, width))] + out_shape
        out_specs = [ANY] + out_specs
    out = pl.pallas_call(
        functools.partial(front_kernel, layer, chunk, pieces),
        grid=(1,),
        out_shape=out_shape,
        in_specs=[SMEM, SMEM, whole((1, width)), table, table] + [ANY] * (len(x_list) + 6) + [small] * (4 * chunk),
        out_specs=out_specs,
        scratch_shapes=[
            pltpu.VMEM((rows, width), BF16),
            pltpu.VMEM((rows, width), BF16),
            pltpu.VMEM((6, width, head), BF16),
            pltpu.VMEM((2, rows, head), BF16),
            pltpu.SemaphoreType.DMA((8,)),
            pltpu.SemaphoreType.DMA((6,)),
            pltpu.SemaphoreType.DMA,
        ],
        compiler_params=pltpu.CompilerParams(vmem_limit_bytes=VMEM),
        cost_estimate=cost(flops, 12 * width * head + 4 * rows * width, 2 * rows * rows * (chunk + 1)),
    )(ids, length, gain, cos_t, sin_t, *x_list, *weights, *[k for group in old for k in group])
    return out if pieces else [None] + list(out)


def back_kernel(chunk, from_hidden, ids_ref, gain_ref, x_ref, *refs):
    refs = list(refs)
    o_refs = [refs.pop(0) for _ in range(8)]
    w_refs = [refs.pop(0) for _ in range(8)]
    ff = [refs.pop(0) for _ in range(6)]
    base = [refs.pop(0) for _ in range(2)]
    sends = [[refs.pop(0) for _ in range(2)] for _ in range(3)]
    x_buf, o_buf, w_buf, normed, acc, x_sem, o_sem, w_sem = refs
    rows, _ = x_buf.shape
    head = o_refs[0].shape[-1]
    part = rows // CHIPS
    step = pl.program_id(0)
    tile = min(ROW_TILE, rows)

    @pl.when(step == 0)
    def _():
        src = x_ref.at[ids_ref[1], pl.ds(chunk * rows, rows)] if from_hidden else x_ref
        x_copy = pltpu.make_async_copy(src, x_buf, x_sem)
        o_copies = [pltpu.make_async_copy(o_refs[n], o_buf.at[:, pl.ds(n * head, head)], o_sem.at[n]) for n in range(8)]
        w_copies = [pltpu.make_async_copy(w_refs[n], w_buf.at[pl.ds(n * head, head)], w_sem.at[n]) for n in range(8)]
        for n in range(8):
            o_copies[n].start()
            w_copies[n].start()
        x_copy.start()
        for group in range(2):
            for n in range(4 * group, 4 * group + 4):
                o_copies[n].wait()
                w_copies[n].wait()
            if group == 1:
                x_copy.wait()
            cut = pl.ds(4 * group * head, 4 * head)
            for r in range(0, rows, tile):
                prod = jnp.dot(o_buf[pl.ds(r, tile), cut], w_buf[cut], preferred_element_type=F32)
                if group == 0:
                    acc[pl.ds(r, tile)] = prod
                else:
                    mid = (x_buf[pl.ds(r, tile)].astype(F32) + (acc[pl.ds(r, tile)] + prod)).astype(BF16)
                    x_buf[pl.ds(r, tile)] = mid
                    normed[pl.ds(r, tile)] = norm_rows(mid.astype(F32), gain_ref[...])

    a = normed[...]
    total = None
    for n in range(2):
        gate = jnp.dot(a, ff[n][...], preferred_element_type=F32)
        up = jnp.dot(a, ff[2 + n][...], preferred_element_type=F32)
        act = (jax.nn.gelu(gate, approximate=True) * up).astype(BF16)
        prod = jnp.dot(act, ff[4 + n][...], preferred_element_type=F32)
        total = prod if total is None else total + prod

    @pl.when(step == 0)
    def _():
        acc[...] = total

    @pl.when(step > 0)
    def _():
        acc[...] += total

    @pl.when(step == pl.num_programs(0) - 1)
    def _():
        for half in range(2):
            own = pl.ds(piece_rows(ids_ref, 0, half, part), part // 2)
            base[half][...] = x_buf[own].astype(F32) + acc[own]
            for place in range(1, 4):
                cut = pl.ds(piece_rows(ids_ref, place, half, part), part // 2)
                sends[place - 1][half][...] = acc[cut].astype(BF16)


def back_call(layer, chunk, ids, gain, x, o_list, w_list, ff_w, rows):
    width = w_list[0].shape[-1]
    head = w_list[0].shape[0]
    ff = ff_w[0].shape[-1]
    tile = min(FF_TILE, ff)
    col = pl.BlockSpec((None, width, tile), lambda i: (layer, 0, i))
    row = pl.BlockSpec((None, tile, width), lambda i: (layer, i, 0))
    half = rows // CHIPS // 2
    return pl.pallas_call(
        functools.partial(back_kernel, chunk, x.ndim == 3),
        grid=(ff // tile,),
        out_shape=[struct((half, width), F32)] * 2 + [struct((half, width))] * 6,
        in_specs=[SMEM, whole((1, width))] + [ANY] * 17 + [col] * 4 + [row] * 2,
        out_specs=[whole((half, width))] * 8,
        scratch_shapes=[
            pltpu.VMEM((rows, width), BF16),
            pltpu.VMEM((rows, 8 * head), BF16),
            pltpu.VMEM((8 * head, width), BF16),
            pltpu.VMEM((rows, width), BF16),
            pltpu.VMEM((rows, width), F32),
            pltpu.SemaphoreType.DMA,
            pltpu.SemaphoreType.DMA((8,)),
            pltpu.SemaphoreType.DMA((8,)),
        ],
        compiler_params=pltpu.CompilerParams(vmem_limit_bytes=VMEM),
        cost_estimate=cost(12 * rows * width * ff + 16 * rows * head * width, 12 * width * ff + 16 * head * width + 8 * rows * width, 2 * rows * ff),
    )(ids, gain, x, *o_list, *w_list, *ff_w)


def place_kernel(chunk, ids_ref, *refs):
    pieces, (h_ref, buf, in_sem, out_sem) = refs[:16], refs[-4:]
    part = 2 * pieces[0].shape[0]
    copies = []
    for n in range(16):
        copies.append(pltpu.make_async_copy(pieces[n], buf.at[n], in_sem.at[n]))
        copies[-1].start()
    outs = []
    for n in range(16):
        prompt = ids_ref[1] if n < 8 else 1 - ids_ref[1]
        at = chunk * part * CHIPS + piece_rows(ids_ref, n % 8 // 2, n % 2, part)
        copies[n].wait()
        outs.append(pltpu.make_async_copy(buf.at[n], h_ref.at[prompt, pl.ds(pl.multiple_of(at, part // 2), part // 2)], out_sem.at[n]))
        outs[-1].start()
    for c in outs:
        c.wait()


def place_call(chunk, ids, pieces, before, shape):
    extra = [] if before is None else [before]
    return pl.pallas_call(
        functools.partial(place_kernel, chunk),
        out_shape=struct(shape),
        in_specs=[SMEM] + [ANY] * (16 + len(extra)),
        out_specs=ANY,
        scratch_shapes=[pltpu.VMEM((16, *pieces[0].shape), BF16), pltpu.SemaphoreType.DMA((16,)), pltpu.SemaphoreType.DMA((16,))],
        input_output_aliases={17: 0} if extra else {},
        compiler_params=pltpu.CompilerParams(vmem_limit_bytes=VMEM),
        cost_estimate=cost(2e9, 1 << 23),
    )(ids, *pieces, *extra)


def rope_tables(seq_len, head_dim):
    half_dim = head_dim // 2
    inv_freq = ROPE_BASE ** (-jnp.arange(half_dim, dtype=F32) * (2.0 / head_dim))
    angles = jnp.arange(seq_len, dtype=F32)[:, None] * inv_freq[None, :]
    return jnp.cos(angles), jnp.sin(angles)


def solution(mesh):
    groups, members = mesh.devices.shape
    chips = members // CORES
    assert chips == CHIPS
    fine = Mesh(mesh.devices.reshape(groups, chips, CORES), ("dp", "x", "core"))
    tp = ("x", "core")

    def swap(value):
        return lax.ppermute(value, "core", [(0, 1), (1, 0)])

    def right(value):
        return lax.ppermute(value, "x", [(i, (i + 1) % chips) for i in range(chips)])

    def left(value):
        return lax.ppermute(value, "x", [((i + 1) % chips, i) for i in range(chips)])

    def gather(a, b):
        ra, rb, la, lb = right(a), right(b), left(a), left(b)
        return [a, b, ra, rb, la, lb, right(ra), left(lb)]

    def add(a, b):
        return (a.astype(F32) + b.astype(F32)).astype(BF16)

    def layers_body(hidden, lengths, w_query, w_key, w_value, w_out, w_gate, w_up, w_down, norm_attn, norm_mlp):
        core = lax.axis_index("core")
        ids = jnp.stack([lax.axis_index("x"), core]).astype(jnp.int32)
        layers = w_query.shape[0]
        _, seq, width = hidden.shape
        head = w_query.shape[-1]
        rows = seq // CHUNKS
        length = lax.dynamic_slice_in_dim(lengths, core, 1)
        cos_t, sin_t = rope_tables(seq, head)
        qkv_w = []
        for w in (w_query, w_key, w_value):
            own = w.reshape(layers, width, head)
            qkv_w += [own, swap(own)]
        ff_w = []
        for w in (w_gate, w_up, w_down):
            ff_w += [w, swap(w)]
        out_w = []
        for l in range(layers):
            own = w_out[l].reshape(head, width)
            from_left, from_right = right(own), left(own)
            far = right(from_left) if l % 2 == 0 else left(from_right)
            mine = [own, from_left, from_right, far]
            out_w.append([w for m in mine for w in (m, swap(m))])
        x = [[hidden]] * CHUNKS
        k_cache, v_cache = [], []
        h_out = None
        for l in range(layers):
            old = [[], [], [], []]
            o_all = []
            for i in range(CHUNKS):
                got = front_call(l, i, ids, length, norm_attn[l][None, :], cos_t, sin_t, x[i], qkv_w, old, rows)
                if l > 0:
                    x[i] = [got[0]]
                old = [group + [k] for group, k in zip(old, got[1:5])]
                o_all.append(gather(*got[5:7]))
            for i in range(CHUNKS):
                out = back_call(l, i, ids, norm_mlp[l][None, :], x[i][0], o_all[i], out_w[l], ff_w, rows)
                base_a, base_b, left_a, left_b, right_a, right_b, far_a, far_b = out
                got_b, got_a = right(right_b), left(left_a)
                to_right = add(right_a, right(far_a))
                to_left = add(left_b, left(far_b))
                new_a = (base_a + right(to_right).astype(F32) + got_a.astype(F32)).astype(BF16)
                new_b = (base_b + got_b.astype(F32) + left(to_left).astype(F32)).astype(BF16)
                x[i] = gather(new_a, new_b)
                if l == layers - 1:
                    h_out = place_call(i, ids, x[i] + [swap(p) for p in x[i]], h_out, hidden.shape)
            for cache, own, other in ((k_cache, old[0], old[1]), (v_cache, old[2], old[3])):
                own = jnp.concatenate(own, axis=0)
                got = swap(jnp.concatenate(other, axis=0))
                cache.append(jnp.where(core == 0, jnp.stack([own, got]), jnp.stack([got, own]))[:, None])
        return h_out, jnp.stack(k_cache), jnp.stack(v_cache)

    head_cols = P(None, None, tp, None)
    step = jax.shard_map(
        layers_body,
        mesh=fine,
        in_specs=(P("dp"), P("dp"), head_cols, head_cols, head_cols, P(None, tp, None, None), P(None, None, tp), P(None, None, tp), P(None, tp, None), P(), P()),
        out_specs=(P("dp"), P(None, "dp", tp), P(None, "dp", tp)),
        check_vma=False,
    )
    return lambda *args: step(*args)
```

```python
import functools

import jax
import jax.numpy as jnp
from jax import lax
from jax.experimental import pallas as pl
from jax.experimental.pallas import tpu as pltpu
from jax.sharding import Mesh
from jax.sharding import PartitionSpec as P


RMS_EPS = 1e-6
ROPE_BASE = 10000.0
CORES = 2
CHIPS = 4
CHUNKS = 4
ROW_TILE = 256
FF_TILE = 256
VMEM = 60 * 1024 * 1024
BF16 = jnp.bfloat16
F32 = jnp.float32
ANY = pl.BlockSpec(memory_space=pl.ANY)
SMEM = pl.BlockSpec(memory_space=pltpu.SMEM)
OFFSETS = (0, 3, 1, 2)
MESH = pl.DeviceIdType.MESH


def cost(flops, nbytes, exps=0):
    return pl.CostEstimate(flops=int(flops), bytes_accessed=int(nbytes), transcendentals=int(exps))


def norm_rows(x_f32, gain):
    mean_sq = jnp.mean(x_f32 * x_f32, axis=-1, keepdims=True)
    return (x_f32 * lax.rsqrt(mean_sq + RMS_EPS) * (1.0 + gain)).astype(BF16)


def struct(shape, dtype=BF16):
    return jax.ShapeDtypeStruct(shape, dtype)


def whole(shape):
    return pl.BlockSpec(shape, lambda *_: (0,) * len(shape))


def piece_rows(place, part):
    return pl.multiple_of(lax.rem(lax.axis_index("x") + OFFSETS[place], CHIPS) * part, part)


def to_right():
    return {"x": lax.rem(lax.axis_index("x") + 1, CHIPS)}


def to_left():
    return {"x": lax.rem(lax.axis_index("x") + CHIPS - 1, CHIPS)}


def to_partner():
    return {"core": 1 - lax.axis_index("core")}


def remote(src, dst, send, recv, device):
    return pltpu.make_async_remote_copy(src_ref=src, dst_ref=dst, send_sem=send, recv_sem=recv, device_id=device, device_id_type=MESH)


class Gather:
    def __init__(self, block):
        self.inputs = [block]
        shape = struct(block.shape, block.dtype)
        self.out_shapes, self.out_specs = [shape] * 3, [ANY] * 3
        self.scratch = [pltpu.SemaphoreType.DMA((4,)), pltpu.SemaphoreType.DMA((4,))]

    def bind(self, inputs, outputs, scratch):
        own, (r, l, f), (send, recv) = inputs[0], outputs, scratch
        half = own.shape[0] // 2
        top, low = pl.ds(0, half), pl.ds(half, half)
        first = lambda: (remote(own, r, send.at[0], recv.at[0], to_right()), remote(own, l, send.at[1], recv.at[1], to_left()))
        second = lambda: (
            remote(r.at[top], f.at[top], send.at[2], recv.at[2], to_right()),
            remote(l.at[low], f.at[low], send.at[3], recv.at[3], to_left()),
        )

        def begin():
            for c in first():
                c.start()

        def onward():
            for a, b in zip(first(), second()):
                a.wait_recv()
                b.start()

        def finish():
            for c in first():
                c.wait_send()
            for c in second():
                c.wait()

        return {0: begin, 2: onward, 3: finish}


class Reduce:
    def __init__(self, base, left, right, far):
        self.inputs = [base, left, right, far]
        rows, width = base.shape
        self.out_shapes, self.out_specs = [struct((rows, width))], [whole((rows, width))]
        half, full = pltpu.VMEM((rows // 2, width), BF16), pltpu.VMEM((rows, width), BF16)
        self.scratch = [half, half, half, half, full, full, pltpu.VMEM((rows, width), F32)]
        self.scratch += [pltpu.SemaphoreType.DMA((6,)), pltpu.SemaphoreType.DMA((6,)), pltpu.SemaphoreType.DMA((3,))]

    def bind(self, inputs, outputs, scratch):
        base, left, right, far = inputs
        t_r, t_l, add_r, add_l, in_r, in_l, base_v, send, recv, load = scratch
        rows = base.shape[0]
        half = rows // 2
        top, low = pl.ds(0, half), pl.ds(half, half)
        first = lambda: (
            remote(far.at[top], t_r, send.at[0], recv.at[0], to_right()),
            remote(far.at[low], t_l, send.at[1], recv.at[1], to_left()),
        )
        direct = lambda: (
            remote(right.at[low], in_r.at[low], send.at[2], recv.at[2], to_right()),
            remote(left.at[top], in_l.at[top], send.at[3], recv.at[3], to_left()),
        )
        second = lambda: (
            remote(add_r, in_r.at[top], send.at[4], recv.at[4], to_right()),
            remote(add_l, in_l.at[low], send.at[5], recv.at[5], to_left()),
        )
        local = lambda: (
            pltpu.make_async_copy(right.at[top], add_r, load.at[0]),
            pltpu.make_async_copy(left.at[low], add_l, load.at[1]),
            pltpu.make_async_copy(base, base_v, load.at[2]),
        )

        def begin():
            for c in (*first(), *direct(), *local()):
                c.start()

        def onward():
            for c in local():
                c.wait()
            for c, add, t in zip(first(), (add_r, add_l), (t_r, t_l)):
                c.wait_recv()
                add[...] = (add[...].astype(F32) + t[...].astype(F32)).astype(BF16)
            for c in second():
                c.start()

        def finish():
            for c in first():
                c.wait_send()
            for c in (*direct(), *second()):
                c.wait()
            outputs[0][...] = (base_v[...] + in_r[...].astype(F32) + in_l[...].astype(F32)).astype(BF16)

        return {0: begin, 1: onward, 3: finish}


class Exchange:
    def __init__(self, blocks):
        self.inputs = list(blocks)
        self.out_shapes, self.out_specs = [struct(b.shape, b.dtype) for b in blocks], [ANY] * len(blocks)
        self.scratch = [pltpu.SemaphoreType.DMA((len(blocks),)), pltpu.SemaphoreType.DMA((len(blocks),))]

    def bind(self, inputs, outputs, scratch):
        send, recv = scratch
        copies = lambda: [remote(a, b, send.at[n], recv.at[n], to_partner()) for n, (a, b) in enumerate(zip(inputs, outputs))]

        def begin():
            for c in copies():
                c.start()

        def finish():
            for c in copies():
                c.wait()

        return {0: begin, 3: finish}


def stage(compute, inputs, in_specs, out_shapes, out_specs, scratch, comms, grid, cost_estimate, ident):
    sizes = [(len(c.inputs), len(c.out_shapes), len(c.scratch)) for c in comms]
    counts = [len(inputs), len(out_shapes), len(scratch)]
    all_in, all_specs = list(inputs), list(in_specs)
    all_shapes, all_outs, all_scratch = list(out_shapes), list(out_specs), list(scratch)
    for c in comms:
        all_in += c.inputs
        all_specs += [ANY] * len(c.inputs)
        all_shapes += c.out_shapes
        all_outs += c.out_specs
        all_scratch += c.scratch
    total_in, total_out = len(all_in), len(all_shapes)
    partner = any(isinstance(c, Exchange) for c in comms)
    ring = any(not isinstance(c, Exchange) for c in comms)

    def kernel(*refs):
        groups = [list(refs[:total_in]), list(refs[total_in : total_in + total_out]), list(refs[total_in + total_out :])]
        mine = [g[:n] for g, n in zip(groups, counts)]
        rest = [g[n:] for g, n in zip(groups, counts)]
        acts = []
        for c, size in zip(comms, sizes):
            acts.append(c.bind(*[g[:n] for g, n in zip(rest, size)]))
            rest = [g[n:] for g, n in zip(rest, size)]

        def at(point):
            if point == 0 and comms:
                barrier = pltpu.get_barrier_semaphore()
                targets = ([to_right(), to_left()] if ring else []) + ([to_partner()] if partner else [])
                for t in targets:
                    pl.semaphore_signal(barrier, inc=1, device_id=t, device_id_type=MESH)
                pl.semaphore_wait(barrier, len(targets))
            for a in acts:
                if point in a:
                    a[point]()

        compute(*mine, at)

    extra = dict(collective_id=ident, has_side_effects=True) if comms else {}
    out = pl.pallas_call(
        kernel,
        grid=grid,
        out_shape=all_shapes,
        in_specs=all_specs,
        out_specs=all_outs,
        scratch_shapes=all_scratch,
        compiler_params=pltpu.CompilerParams(vmem_limit_bytes=VMEM, **extra),
        cost_estimate=cost_estimate,
    )(*all_in)
    made = list(out[: counts[1]])
    rest = list(out[counts[1] :])
    results = []
    for _, n, _ in sizes:
        results.append(rest[:n])
        rest = rest[n:]
    return made, results


def front_body(layer, chunk, pieces, inputs, outputs, scratch, at):
    at(0)
    refs = list(inputs)
    len_ref, gain_ref, cos_ref, sin_ref = (refs.pop(0) for _ in range(4))
    x_refs = [refs.pop(0) for _ in range(CHIPS if pieces else 1)]
    w_refs = [refs.pop(0) for _ in range(6)]
    old = [[refs.pop(0) for _ in range(chunk)] for _ in range(4)]
    new, o_ref = outputs[:4], outputs[4]
    x_buf, normed, w_buf, q_buf, x_sem, w_sem, out_sem = scratch
    rows, _ = x_buf.shape
    head = q_buf.shape[-1]
    half = head // 2
    if pieces:
        part = rows // CHIPS
        copies = [pltpu.make_async_copy(x_refs[n], x_buf.at[pl.ds(piece_rows(n, part), part)], x_sem.at[n]) for n in range(CHIPS)]
    else:
        copies = [pltpu.make_async_copy(x_refs[0].at[lax.axis_index("core"), pl.ds(chunk * rows, rows)], x_buf, x_sem.at[0])]
    for c in copies:
        c.start()
    loads = [pltpu.make_async_copy(w_refs[n].at[layer], w_buf.at[n], w_sem.at[n]) for n in range(6)]
    for c in loads:
        c.start()
    for c in copies:
        c.wait()
    save = None
    if pieces:
        save = pltpu.make_async_copy(x_buf, outputs[5], out_sem)
        save.start()
    tile = min(ROW_TILE, rows)
    for r in range(0, rows, tile):
        normed[pl.ds(r, tile)] = norm_rows(x_buf[pl.ds(r, tile)].astype(F32), gain_ref[...])

    def rope(y, r):
        low, high = y[:, :half], y[:, half:]
        c, s = cos_ref[pl.ds(r, tile)], sin_ref[pl.ds(r, tile)]
        return jnp.concatenate([low * c - high * s, high * c + low * s], axis=-1)

    for n in range(6):
        loads[n].wait()
        for r in range(0, rows, tile):
            y = jnp.dot(normed[pl.ds(r, tile)], w_buf[n], preferred_element_type=F32)
            if n < 2:
                q_buf[n, pl.ds(r, tile)] = (rope(y, r) * head**-0.5).astype(BF16)
            elif n < 4:
                new[n - 2][pl.ds(r, tile)] = rope(y, r).astype(BF16)
            else:
                new[n - 2][pl.ds(r, tile)] = y.astype(BF16)
    at(1)
    dims = (((1,), (1,)), ((), ()))
    length = len_ref[0]
    col = lax.broadcasted_iota(jnp.int32, (1, rows), 1)
    lower = lax.broadcasted_iota(jnp.int32, (tile, rows), 1) - lax.broadcasted_iota(jnp.int32, (tile, rows), 0)
    bias = [jnp.where(col < length - j * rows, 0.0, -1e30).astype(F32) for j in range(chunk + 1)]
    for h in range(2):
        keys = old[h] + [new[h]]
        values = old[2 + h] + [new[2 + h]]
        for r in range(0, rows, tile):
            query = q_buf[h, pl.ds(r, tile)]
            blocks = []
            for j in range(chunk + 1):
                scores = lax.dot_general(query, keys[j][...], dims, preferred_element_type=F32) + bias[j]
                if j == chunk:
                    scores = jnp.where(lower <= r, scores, -1e30)
                blocks.append(scores)
            top = functools.reduce(jnp.maximum, [jnp.max(b, axis=-1, keepdims=True) for b in blocks])
            blocks = [jnp.exp(b - top) for b in blocks]
            inv = 1.0 / functools.reduce(jnp.add, [jnp.sum(b, axis=-1, keepdims=True) for b in blocks])
            total = None
            for j in range(chunk + 1):
                prod = jnp.dot((blocks[j] * inv).astype(BF16), values[j][...], preferred_element_type=F32)
                total = prod if total is None else total + prod
            o_ref[pl.ds(r, tile), pl.ds(h * head, head)] = total.astype(BF16)
        if h == 0:
            at(2)
    if save is not None:
        save.wait()
    at(3)


def front_call(layer, chunk, length, gain, cos_t, sin_t, x_list, weights, old, rows, comms, ident):
    width, head = weights[0].shape[1:]
    pieces = len(x_list) > 1
    small = whole((rows, head))
    table = pl.BlockSpec((rows, head // 2), lambda *_: (chunk, 0))
    flops = 12 * rows * width * head + 8 * rows * rows * (chunk + 1) * head
    shapes, specs = [struct((rows, head))] * 4 + [struct((rows, 2 * head))], [small] * 4 + [whole((rows, 2 * head))]
    if pieces:
        shapes, specs = shapes + [struct((rows, width))], specs + [ANY]
    return stage(
        functools.partial(front_body, layer, chunk, pieces),
        [length, gain, cos_t, sin_t, *x_list, *weights, *[k for group in old for k in group]],
        [SMEM, whole((1, width)), table, table] + [ANY] * (len(x_list) + 6) + [small] * (4 * chunk),
        shapes,
        specs,
        [
            pltpu.VMEM((rows, width), BF16),
            pltpu.VMEM((rows, width), BF16),
            pltpu.VMEM((6, width, head), BF16),
            pltpu.VMEM((2, rows, head), BF16),
            pltpu.SemaphoreType.DMA((CHIPS,)),
            pltpu.SemaphoreType.DMA((6,)),
            pltpu.SemaphoreType.DMA,
        ],
        comms,
        (1,),
        cost(flops, 12 * width * head + 4 * rows * width, 2 * rows * rows * (chunk + 1)),
        ident,
    )


def back_body(chunk, from_hidden, inputs, outputs, scratch, at):
    gain_ref, x_ref = inputs[:2]
    o_refs, w_refs, ff = inputs[2:6], inputs[6:14], inputs[14:]
    x_buf, o_buf, w_buf, normed, acc, x_sem, o_sem, w_sem = scratch
    rows, _ = x_buf.shape
    inner = o_refs[0].shape[-1]
    head = w_refs[0].shape[0]
    part = rows // CHIPS
    step = pl.program_id(0)
    tile = min(ROW_TILE, rows)

    @pl.when(step == 0)
    def _():
        src = x_ref.at[lax.axis_index("core"), pl.ds(chunk * rows, rows)] if from_hidden else x_ref
        x_copy = pltpu.make_async_copy(src, x_buf, x_sem)
        o_copies = [pltpu.make_async_copy(o_refs[n], o_buf.at[:, pl.ds(n * inner, inner)], o_sem.at[n]) for n in range(CHIPS)]
        w_copies = [pltpu.make_async_copy(w_refs[n], w_buf.at[pl.ds(n * head, head)], w_sem.at[n]) for n in range(8)]
        for n in range(CHIPS):
            o_copies[n].start()
            w_copies[2 * n].start()
            w_copies[2 * n + 1].start()
        x_copy.start()
        at(0)
        for group in range(2):
            for n in range(2 * group, 2 * group + 2):
                o_copies[n].wait()
                w_copies[2 * n].wait()
                w_copies[2 * n + 1].wait()
            if group == 1:
                x_copy.wait()
            cut = pl.ds(2 * group * inner, 2 * inner)
            for r in range(0, rows, tile):
                prod = jnp.dot(o_buf[pl.ds(r, tile), cut], w_buf[cut], preferred_element_type=F32)
                if group == 0:
                    acc[pl.ds(r, tile)] = prod
                else:
                    mid = (x_buf[pl.ds(r, tile)].astype(F32) + (acc[pl.ds(r, tile)] + prod)).astype(BF16)
                    x_buf[pl.ds(r, tile)] = mid
                    normed[pl.ds(r, tile)] = norm_rows(mid.astype(F32), gain_ref[...])

    @pl.when(step == 1)
    def _():
        at(1)

    @pl.when(step == pl.num_programs(0) - 1)
    def _():
        at(2)

    a = normed[...]
    total = None
    for n in range(2):
        gate = jnp.dot(a, ff[n][...], preferred_element_type=F32)
        up = jnp.dot(a, ff[2 + n][...], preferred_element_type=F32)
        act = (jax.nn.gelu(gate, approximate=True) * up).astype(BF16)
        prod = jnp.dot(act, ff[4 + n][...], preferred_element_type=F32)
        total = prod if total is None else total + prod

    @pl.when(step == 0)
    def _():
        acc[...] = total

    @pl.when(step > 0)
    def _():
        acc[...] += total

    @pl.when(step == pl.num_programs(0) - 1)
    def _():
        own = pl.ds(piece_rows(0, part), part)
        outputs[0][...] = x_buf[own].astype(F32) + acc[own]
        for place in range(1, CHIPS):
            outputs[place][...] = acc[pl.ds(piece_rows(place, part), part)].astype(BF16)
        at(3)


def back_call(layer, chunk, gain, x, o_list, w_list, ff_w, rows, comms, ident):
    head, width = w_list[0].shape
    ff = ff_w[0].shape[-1]
    tile = min(FF_TILE, ff)
    col = pl.BlockSpec((None, width, tile), lambda i: (layer, 0, i))
    row = pl.BlockSpec((None, tile, width), lambda i: (layer, i, 0))
    part = rows // CHIPS
    return stage(
        functools.partial(back_body, chunk, x.ndim == 3),
        [gain, x, *o_list, *w_list, *ff_w],
        [whole((1, width))] + [ANY] * 13 + [col] * 4 + [row] * 2,
        [struct((part, width), F32)] + [struct((part, width))] * 3,
        [whole((part, width))] * 4,
        [
            pltpu.VMEM((rows, width), BF16),
            pltpu.VMEM((rows, 8 * head), BF16),
            pltpu.VMEM((8 * head, width), BF16),
            pltpu.VMEM((rows, width), BF16),
            pltpu.VMEM((rows, width), F32),
            pltpu.SemaphoreType.DMA,
            pltpu.SemaphoreType.DMA((CHIPS,)),
            pltpu.SemaphoreType.DMA((8,)),
        ],
        comms,
        (ff // tile,),
        cost(12 * rows * width * ff + 16 * rows * head * width, 12 * width * ff + 16 * head * width + 8 * rows * width, 2 * rows * ff),
        ident,
    )


def idle_body(inputs, outputs, scratch, at):
    for point in range(4):
        at(point)


def idle_call(comms, ident):
    return stage(idle_body, [], [], [], [], [], comms, (1,), cost(2e10, 1 << 22), ident)[1]


def place_kernel(*refs):
    h_ref, buf, in_sem, out_sem = refs[-4:]
    pieces = refs[:-4]
    part = pieces[0].shape[0]
    depth = buf.shape[0]
    core = lax.axis_index("core")
    count = len(pieces)
    loads, saves = [], []
    for n in range(count):
        chunk, rest = divmod(n, 2 * CHIPS)
        prompt = core if rest < CHIPS else 1 - core
        at = pl.multiple_of(chunk * part * CHIPS + piece_rows(rest % CHIPS, part), part)
        loads.append(pltpu.make_async_copy(pieces[n], buf.at[n % depth], in_sem.at[n % depth]))
        saves.append(pltpu.make_async_copy(buf.at[n % depth], h_ref.at[prompt, pl.ds(at, part)], out_sem.at[n % depth]))
    for n in range(depth):
        loads[n].start()
    for n in range(count):
        loads[n].wait()
        saves[n].start()
        m = n - depth // 2
        if m >= 0 and m + depth < count:
            saves[m].wait()
            loads[m + depth].start()
    for n in range(max(0, count - depth), count):
        saves[n].wait()


def place_call(pieces, shape):
    depth = min(16, len(pieces))
    return pl.pallas_call(
        place_kernel,
        out_shape=struct(shape),
        in_specs=[ANY] * len(pieces),
        out_specs=ANY,
        scratch_shapes=[pltpu.VMEM((depth, *pieces[0].shape), BF16), pltpu.SemaphoreType.DMA((depth,)), pltpu.SemaphoreType.DMA((depth,))],
        compiler_params=pltpu.CompilerParams(vmem_limit_bytes=VMEM),
        cost_estimate=cost(1e10, 1 << 25),
    )(*pieces)


def rope_tables(seq_len, head_dim):
    half_dim = head_dim // 2
    inv_freq = ROPE_BASE ** (-jnp.arange(half_dim, dtype=F32) * (2.0 / head_dim))
    angles = jnp.arange(seq_len, dtype=F32)[:, None] * inv_freq[None, :]
    return jnp.cos(angles), jnp.sin(angles)


def solution(mesh):
    groups, members = mesh.devices.shape
    chips = members // CORES
    assert chips == CHIPS
    fine = Mesh(mesh.devices.reshape(groups, chips, CORES), ("dp", "x", "core"))
    tp = ("x", "core")

    def swap(value):
        return lax.ppermute(value, "core", [(0, 1), (1, 0)])

    def right(value):
        return lax.ppermute(value, "x", [(i, (i + 1) % chips) for i in range(chips)])

    def left(value):
        return lax.ppermute(value, "x", [((i + 1) % chips, i) for i in range(chips)])

    def layers_body(hidden, lengths, w_query, w_key, w_value, w_out, w_gate, w_up, w_down, norm_attn, norm_mlp):
        core = lax.axis_index("core")
        layers = w_query.shape[0]
        _, seq, width = hidden.shape
        head = w_query.shape[-1]
        rows = seq // CHUNKS
        length = lax.dynamic_slice_in_dim(lengths, core, 1)
        cos_t, sin_t = rope_tables(seq, head)
        qkv_w = []
        for w in (w_query, w_key, w_value):
            own = w.reshape(layers, width, head)
            qkv_w += [own, swap(own)]
        ff_w = []
        for w in (w_gate, w_up, w_down):
            ff_w += [w, swap(w)]
        out_w = []
        for l in range(layers):
            own = w_out[l].reshape(head, width)
            from_left, from_right = right(own), left(own)
            far = right(from_left) if l % 2 == 0 else left(from_right)
            mine = [own, from_left, from_right, far]
            out_w.append([w for m in mine for w in (m, swap(m))])
        x = [[hidden]] * CHUNKS
        k_cache, v_cache = [], []
        waiting = []
        ident = iter(range(1000))
        other = [None] * CHUNKS

        def carry(call):
            now = [make() for make, _ in waiting]
            sinks = [sink for _, sink in waiting]
            waiting.clear()
            made, results = call(now, next(ident))
            for sink, result in zip(sinks, results):
                sink(result)
            return made

        def send_x(i, block, final):
            def landed(blocks):
                x[i] = [block, *blocks]
                if final:
                    waiting.append((lambda: Exchange(x[i]), functools.partial(other.__setitem__, i)))

            waiting.append((lambda: Gather(block), landed))

        def send_sum(i, parts, final):
            waiting.append((lambda: Reduce(*parts), lambda got: send_x(i, got[0], final)))

        for l in range(layers):
            final = l == layers - 1
            old = [[], [], [], []]
            o_all = [None] * CHUNKS
            for i in range(CHUNKS):
                made = carry(
                    lambda comms, n: front_call(l, i, length, norm_attn[l][None, :], cos_t, sin_t, x[i], qkv_w, old, rows, comms, n)
                )
                old = [group + [k] for group, k in zip(old, made[:4])]
                o = made[4]
                if l > 0:
                    x[i] = [made[5]]
                waiting.append((lambda o=o: Gather(o), lambda got, i=i, o=o: o_all.__setitem__(i, [o, *got])))
            for i in range(CHUNKS):
                made = carry(
                    lambda comms, n: back_call(l, i, norm_mlp[l][None, :], x[i][0], o_all[i], out_w[l], ff_w, rows, comms, n)
                )
                send_sum(i, made, final)
            for cache, own, theirs in ((k_cache, old[0], old[1]), (v_cache, old[2], old[3])):
                own = jnp.concatenate(own, axis=0)
                got = swap(jnp.concatenate(theirs, axis=0))
                cache.append(jnp.where(core == 0, jnp.stack([own, got]), jnp.stack([got, own]))[:, None])
        while waiting:
            carry(lambda comms, n: ([], idle_call(comms, n)))
        h_out = place_call([p for i in range(CHUNKS) for p in (*x[i], *other[i])], hidden.shape)
        return h_out, jnp.stack(k_cache), jnp.stack(v_cache)

    head_cols = P(None, None, tp, None)
    step = jax.shard_map(
        layers_body,
        mesh=fine,
        in_specs=(P("dp"), P("dp"), head_cols, head_cols, head_cols, P(None, tp, None, None), P(None, None, tp), P(None, None, tp), P(None, tp, None), P(), P()),
        out_specs=(P("dp"), P(None, "dp", tp), P(None, "dp", tp)),
        check_vma=False,
    )
    return lambda *args: step(*args)
```

```python
import functools

import jax
import jax.numpy as jnp
from jax import lax
from jax.experimental import pallas as pl
from jax.experimental.pallas import tpu as pltpu
from jax.sharding import Mesh
from jax.sharding import PartitionSpec as P


RMS_EPS = 1e-6
ROPE_BASE = 10000.0
CORES = 2
CHIPS = 4
CHUNKS = 4
ROW_TILE = 256
FF_TILE = 256
VMEM = 60 * 1024 * 1024
BF16 = jnp.bfloat16
F32 = jnp.float32
ANY = pl.BlockSpec(memory_space=pl.ANY)
SMEM = pl.BlockSpec(memory_space=pltpu.SMEM)
OFFSETS = (0, 3, 1, 2)
MESH = pl.DeviceIdType.MESH


def cost(flops, nbytes, exps=0):
    return pl.CostEstimate(flops=int(flops), bytes_accessed=int(nbytes), transcendentals=int(exps))


def norm_rows(x_f32, gain):
    mean_sq = jnp.mean(x_f32 * x_f32, axis=-1, keepdims=True)
    return (x_f32 * lax.rsqrt(mean_sq + RMS_EPS) * (1.0 + gain)).astype(BF16)


def struct(shape, dtype=BF16):
    return jax.ShapeDtypeStruct(shape, dtype)


def whole(shape):
    return pl.BlockSpec(shape, lambda *_: (0,) * len(shape))


def piece_rows(place, part):
    return pl.multiple_of(lax.rem(lax.axis_index("x") + OFFSETS[place], CHIPS) * part, part)


def to_right():
    return {"x": lax.rem(lax.axis_index("x") + 1, CHIPS)}


def to_left():
    return {"x": lax.rem(lax.axis_index("x") + CHIPS - 1, CHIPS)}


def remote(src, dst, send, recv, device):
    return pltpu.make_async_remote_copy(src_ref=src, dst_ref=dst, send_sem=send, recv_sem=recv, device_id=device, device_id_type=MESH)


class Gather:
    def __init__(self, block):
        self.inputs = [block]
        shape = struct(block.shape, block.dtype)
        self.out_shapes, self.out_specs = [shape] * 3, [ANY] * 3
        self.scratch = [pltpu.SemaphoreType.DMA((6,)), pltpu.SemaphoreType.DMA((6,))]

    def bind(self, inputs, outputs, scratch):
        own, (r, l, f), (send, recv) = inputs[0], outputs, scratch
        half = own.shape[0] // 2
        top, low = pl.ds(0, half), pl.ds(half, half)
        first = lambda: (
            remote(own.at[top], r.at[top], send.at[0], recv.at[0], to_right()),
            remote(own.at[low], l.at[low], send.at[1], recv.at[1], to_left()),
        )
        rest = lambda: (
            remote(own.at[low], r.at[low], send.at[4], recv.at[4], to_right()),
            remote(own.at[top], l.at[top], send.at[5], recv.at[5], to_left()),
        )
        second = lambda: (
            remote(r.at[top], f.at[top], send.at[2], recv.at[2], to_right()),
            remote(l.at[low], f.at[low], send.at[3], recv.at[3], to_left()),
        )

        def begin():
            for c in (*first(), *rest()):
                c.start()

        def onward():
            for a, b in zip(first(), second()):
                a.wait_recv()
                b.start()

        def finish():
            for c in first():
                c.wait_send()
            for c in (*rest(), *second()):
                c.wait()

        return {0: begin, 1: onward, 3: finish}


class Reduce:
    def __init__(self, base, left, right, far):
        self.inputs = [base, left, right, far]
        rows, width = base.shape
        self.out_shapes, self.out_specs = [struct((rows, width))], [whole((rows, width))]
        half, full = pltpu.VMEM((rows // 2, width), BF16), pltpu.VMEM((rows, width), BF16)
        self.scratch = [half, half, half, half, full, full, pltpu.VMEM((rows, width), F32)]
        self.scratch += [pltpu.SemaphoreType.DMA((6,)), pltpu.SemaphoreType.DMA((6,)), pltpu.SemaphoreType.DMA((3,))]

    def bind(self, inputs, outputs, scratch):
        base, left, right, far = inputs
        t_r, t_l, add_r, add_l, in_r, in_l, base_v, send, recv, load = scratch
        rows = base.shape[0]
        half = rows // 2
        top, low = pl.ds(0, half), pl.ds(half, half)
        first = lambda: (
            remote(far.at[top], t_r, send.at[0], recv.at[0], to_right()),
            remote(far.at[low], t_l, send.at[1], recv.at[1], to_left()),
        )
        direct = lambda: (
            remote(right.at[low], in_r.at[low], send.at[2], recv.at[2], to_right()),
            remote(left.at[top], in_l.at[top], send.at[3], recv.at[3], to_left()),
        )
        second = lambda: (
            remote(add_r, in_r.at[top], send.at[4], recv.at[4], to_right()),
            remote(add_l, in_l.at[low], send.at[5], recv.at[5], to_left()),
        )
        local = lambda: (
            pltpu.make_async_copy(right.at[top], add_r, load.at[0]),
            pltpu.make_async_copy(left.at[low], add_l, load.at[1]),
            pltpu.make_async_copy(base, base_v, load.at[2]),
        )

        def begin():
            for c in (*first(), *direct(), *local()):
                c.start()

        def onward():
            for c in local():
                c.wait()
            for c, add, t in zip(first(), (add_r, add_l), (t_r, t_l)):
                c.wait_recv()
                add[...] = (add[...].astype(F32) + t[...].astype(F32)).astype(BF16)
            for c in second():
                c.start()

        def finish():
            for c in first():
                c.wait_send()
            for c in (*direct(), *second()):
                c.wait()
            outputs[0][...] = (base_v[...] + in_r[...].astype(F32) + in_l[...].astype(F32)).astype(BF16)

        return {0: begin, 1: onward, 3: finish}


def stage(compute, inputs, in_specs, out_shapes, out_specs, scratch, comms, grid, cost_estimate, ident):
    sizes = [(len(c.inputs), len(c.out_shapes), len(c.scratch)) for c in comms]
    counts = [len(inputs), len(out_shapes), len(scratch)]
    all_in, all_specs = list(inputs), list(in_specs)
    all_shapes, all_outs, all_scratch = list(out_shapes), list(out_specs), list(scratch)
    for c in comms:
        all_in += c.inputs
        all_specs += [ANY] * len(c.inputs)
        all_shapes += c.out_shapes
        all_outs += c.out_specs
        all_scratch += c.scratch
    total_in, total_out = len(all_in), len(all_shapes)

    def kernel(*refs):
        groups = [list(refs[:total_in]), list(refs[total_in : total_in + total_out]), list(refs[total_in + total_out :])]
        mine = [g[:n] for g, n in zip(groups, counts)]
        rest = [g[n:] for g, n in zip(groups, counts)]
        acts = []
        for c, size in zip(comms, sizes):
            acts.append(c.bind(*[g[:n] for g, n in zip(rest, size)]))
            rest = [g[n:] for g, n in zip(rest, size)]

        def at(point):
            if point == 0 and comms:
                barrier = pltpu.get_barrier_semaphore()
                targets = [to_right(), to_left()]
                for t in targets:
                    pl.semaphore_signal(barrier, inc=1, device_id=t, device_id_type=MESH)
                pl.semaphore_wait(barrier, len(targets))
            for a in acts:
                if point in a:
                    a[point]()

        compute(*mine, at)

    extra = dict(collective_id=ident, has_side_effects=True) if comms else {}
    out = pl.pallas_call(
        kernel,
        grid=grid,
        out_shape=all_shapes,
        in_specs=all_specs,
        out_specs=all_outs,
        scratch_shapes=all_scratch,
        compiler_params=pltpu.CompilerParams(vmem_limit_bytes=VMEM, **extra),
        cost_estimate=cost_estimate,
    )(*all_in)
    made = list(out[: counts[1]])
    rest = list(out[counts[1] :])
    results = []
    for _, n, _ in sizes:
        results.append(rest[:n])
        rest = rest[n:]
    return made, results


def front_body(layer, chunk, from_hidden, inputs, outputs, scratch, at):
    at(0)
    refs = list(inputs)
    len_ref, gain_ref, cos_ref, sin_ref, x_ref = (refs.pop(0) for _ in range(5))
    w_refs = [refs.pop(0) for _ in range(6)]
    old = [[refs.pop(0) for _ in range(chunk)] for _ in range(4)]
    new, o_ref = outputs[:4], outputs[4]
    x_buf, normed, w_buf, q_buf, x_sem, w_sem = scratch
    rows, _ = x_buf.shape
    head = q_buf.shape[-1]
    half = head // 2
    x_copy = pltpu.make_async_copy(x_ref.at[lax.axis_index("core"), pl.ds(chunk * rows, rows)] if from_hidden else x_ref, x_buf, x_sem)
    x_copy.start()
    loads = [pltpu.make_async_copy(w_refs[n].at[layer], w_buf.at[n], w_sem.at[n]) for n in range(6)]
    for c in loads:
        c.start()
    x_copy.wait()
    tile = min(ROW_TILE, rows)
    for r in range(0, rows, tile):
        normed[pl.ds(r, tile)] = norm_rows(x_buf[pl.ds(r, tile)].astype(F32), gain_ref[...])

    def rope(y, r):
        low, high = y[:, :half], y[:, half:]
        c, s = cos_ref[pl.ds(r, tile)], sin_ref[pl.ds(r, tile)]
        return jnp.concatenate([low * c - high * s, high * c + low * s], axis=-1)

    for n in range(6):
        loads[n].wait()
        for r in range(0, rows, tile):
            y = jnp.dot(normed[pl.ds(r, tile)], w_buf[n], preferred_element_type=F32)
            if n < 2:
                q_buf[n, pl.ds(r, tile)] = (rope(y, r) * head**-0.5).astype(BF16)
            elif n < 4:
                new[n - 2][pl.ds(r, tile)] = rope(y, r).astype(BF16)
            else:
                new[n - 2][pl.ds(r, tile)] = y.astype(BF16)
    at(1)
    dims = (((1,), (1,)), ((), ()))
    length = len_ref[0]
    col = lax.broadcasted_iota(jnp.int32, (1, rows), 1)
    lower = lax.broadcasted_iota(jnp.int32, (tile, rows), 1) - lax.broadcasted_iota(jnp.int32, (tile, rows), 0)
    bias = [jnp.where(col < length - j * rows, 0.0, -1e30).astype(F32) for j in range(chunk + 1)]
    for h in range(2):
        keys = old[h] + [new[h]]
        values = old[2 + h] + [new[2 + h]]
        for r in range(0, rows, tile):
            query = q_buf[h, pl.ds(r, tile)]
            blocks = []
            for j in range(chunk + 1):
                scores = lax.dot_general(query, keys[j][...], dims, preferred_element_type=F32) + bias[j]
                if j == chunk:
                    scores = jnp.where(lower <= r, scores, -1e30)
                blocks.append(scores)
            top = functools.reduce(jnp.maximum, [jnp.max(b, axis=-1, keepdims=True) for b in blocks])
            blocks = [jnp.exp(b - top) for b in blocks]
            inv = 1.0 / functools.reduce(jnp.add, [jnp.sum(b, axis=-1, keepdims=True) for b in blocks])
            total = None
            for j in range(chunk + 1):
                prod = jnp.dot((blocks[j] * inv).astype(BF16), values[j][...], preferred_element_type=F32)
                total = prod if total is None else total + prod
            o_ref[pl.ds(r, tile), pl.ds(h * head, head)] = total.astype(BF16)
        if h == 0:
            at(2)
    at(3)


def front_call(layer, chunk, length, gain, cos_t, sin_t, x, weights, old, rows, comms, ident):
    width, head = weights[0].shape[1:]
    small = whole((rows, head))
    table = pl.BlockSpec((rows, head // 2), lambda *_: (chunk, 0))
    flops = 12 * rows * width * head + 8 * rows * rows * (chunk + 1) * head
    shapes, specs = [struct((rows, head))] * 4 + [struct((rows, 2 * head))], [small] * 4 + [whole((rows, 2 * head))]
    return stage(
        functools.partial(front_body, layer, chunk, x.ndim == 3),
        [length, gain, cos_t, sin_t, x, *weights, *[k for group in old for k in group]],
        [SMEM, whole((1, width)), table, table] + [ANY] * 7 + [small] * (4 * chunk),
        shapes,
        specs,
        [
            pltpu.VMEM((rows, width), BF16),
            pltpu.VMEM((rows, width), BF16),
            pltpu.VMEM((6, width, head), BF16),
            pltpu.VMEM((2, rows, head), BF16),
            pltpu.SemaphoreType.DMA,
            pltpu.SemaphoreType.DMA((6,)),
        ],
        comms,
        (1,),
        cost(flops, 12 * width * head + 4 * rows * width, 2 * rows * rows * (chunk + 1)),
        ident,
    )


def back_body(layer, chunk, from_hidden, inputs, outputs, scratch, at):
    gain_ref, x_ref = inputs[:2]
    o_refs, w_refs, ff, down_refs = inputs[2:6], inputs[6:8], inputs[8:12], inputs[12:]
    x_buf, o_buf, w_buf, normed, acc, act, down, x_sem, o_sem, w_sem, down_sem = scratch
    rows, _ = x_buf.shape
    inner = o_refs[0].shape[-1]
    head = inner // 2
    part = rows // CHIPS
    step = pl.program_id(0)
    tile = min(ROW_TILE, rows)
    cut_ff = ff[0].shape[-1]
    ff_rows = down.shape[0] // 2
    down_copies = [pltpu.make_async_copy(down_refs[n].at[layer], down.at[pl.ds(n * ff_rows, ff_rows)], down_sem.at[n]) for n in range(2)]

    @pl.when(step == 0)
    def _():
        src = x_ref.at[lax.axis_index("core"), pl.ds(chunk * rows, rows)] if from_hidden else x_ref
        x_copy = pltpu.make_async_copy(src, x_buf, x_sem)
        o_copies = [pltpu.make_async_copy(o_refs[n], o_buf.at[:, pl.ds(n * inner, inner)], o_sem.at[n]) for n in range(CHIPS)]
        w_copies = []
        for n in range(CHIPS):
            whose = lax.rem(lax.axis_index("x") + OFFSETS[n], CHIPS)
            for k in range(2):
                w_copies.append(
                    pltpu.make_async_copy(w_refs[k].at[whose], w_buf.at[pl.ds(n * inner + k * head, head)], w_sem.at[2 * n + k])
                )
        for n in range(CHIPS):
            o_copies[n].start()
            w_copies[2 * n].start()
            w_copies[2 * n + 1].start()
        x_copy.start()
        at(0)
        for c in down_copies:
            c.start()
        for group in range(2):
            for n in range(2 * group, 2 * group + 2):
                o_copies[n].wait()
                w_copies[2 * n].wait()
                w_copies[2 * n + 1].wait()
            if group == 1:
                x_copy.wait()
            cut = pl.ds(2 * group * inner, 2 * inner)
            for r in range(0, rows, tile):
                prod = jnp.dot(o_buf[pl.ds(r, tile), cut], w_buf[cut], preferred_element_type=F32)
                if group == 0:
                    acc[pl.ds(r, tile)] = prod
                else:
                    mid = (x_buf[pl.ds(r, tile)].astype(F32) + (acc[pl.ds(r, tile)] + prod)).astype(BF16)
                    x_buf[pl.ds(r, tile)] = mid
                    normed[pl.ds(r, tile)] = norm_rows(mid.astype(F32), gain_ref[...])

    @pl.when(step == 1)
    def _():
        at(1)

    for n in range(2):
        columns = pl.ds(pl.multiple_of(n * ff_rows + step * cut_ff, cut_ff), cut_ff)
        for r in range(0, rows, tile):
            a = normed[pl.ds(r, tile)]
            gate = jnp.dot(a, ff[n][...], preferred_element_type=F32)
            up = jnp.dot(a, ff[2 + n][...], preferred_element_type=F32)
            act[pl.ds(r, tile), columns] = (jax.nn.gelu(gate, approximate=True) * up).astype(BF16)

    @pl.when(step == pl.num_programs(0) - 1)
    def _():
        for c in down_copies:
            c.wait()
        for r in range(0, rows, tile):
            acc[pl.ds(r, tile)] = jnp.dot(act[pl.ds(r, tile)], down[...], preferred_element_type=F32)
        own = pl.ds(piece_rows(0, part), part)
        outputs[0][...] = x_buf[own].astype(F32) + acc[own]
        for place in range(1, CHIPS):
            outputs[place][...] = acc[pl.ds(piece_rows(place, part), part)].astype(BF16)
        at(3)


def back_call(layer, chunk, gain, x, o_list, w_list, ff_w, rows, comms, ident):
    head, width = w_list[0].shape[1:]
    ff = ff_w[0].shape[-1]
    tile = min(FF_TILE, ff)
    col = pl.BlockSpec((None, width, tile), lambda i: (layer, 0, i))
    part = rows // CHIPS
    return stage(
        functools.partial(back_body, layer, chunk, x.ndim == 3),
        [gain, x, *o_list, *w_list, *ff_w],
        [whole((1, width))] + [ANY] * 7 + [col] * 4 + [ANY] * 2,
        [struct((part, width), F32)] + [struct((part, width))] * 3,
        [whole((part, width))] * 4,
        [
            pltpu.VMEM((rows, width), BF16),
            pltpu.VMEM((rows, 8 * head), BF16),
            pltpu.VMEM((8 * head, width), BF16),
            pltpu.VMEM((rows, width), BF16),
            pltpu.VMEM((rows, width), F32),
            pltpu.VMEM((rows, 2 * ff), BF16),
            pltpu.VMEM((2 * ff, width), BF16),
            pltpu.SemaphoreType.DMA,
            pltpu.SemaphoreType.DMA((CHIPS,)),
            pltpu.SemaphoreType.DMA((8,)),
            pltpu.SemaphoreType.DMA((2,)),
        ],
        comms,
        (ff // tile,),
        cost(12 * rows * width * ff + 16 * rows * head * width, 12 * width * ff + 16 * head * width + 8 * rows * width, 2 * rows * ff),
        ident,
    )


def idle_body(inputs, outputs, scratch, at):
    for point in range(4):
        at(point)


def idle_call(comms, ident):
    return stage(idle_body, [], [], [], [], [], comms, (1,), cost(2e10, 1 << 22), ident)[1]


def place_kernel(chunk, both_ref, *refs):
    h_ref, buf, in_sem, out_sem = refs[-4:]
    part = both_ref.shape[2]
    spots = [(c, k) for c in range(CHIPS) for k in range(CORES)]
    loads = [pltpu.make_async_copy(both_ref.at[c, k], buf.at[n], in_sem.at[n]) for n, (c, k) in enumerate(spots)]
    saves = [
        pltpu.make_async_copy(buf.at[n], h_ref.at[k, pl.ds((chunk * CHIPS + c) * part, part)], out_sem.at[n])
        for n, (c, k) in enumerate(spots)
    ]
    for copy in loads:
        copy.start()
    for load, save in zip(loads, saves):
        load.wait()
        save.start()
    for copy in saves:
        copy.wait()


def place_call(chunk, both, before, shape):
    extra = [] if before is None else [before]
    count = CHIPS * CORES
    return pl.pallas_call(
        functools.partial(place_kernel, chunk),
        out_shape=struct(shape),
        in_specs=[ANY] * (1 + len(extra)),
        out_specs=ANY,
        scratch_shapes=[pltpu.VMEM((count, *both.shape[2:]), BF16), pltpu.SemaphoreType.DMA((count,)), pltpu.SemaphoreType.DMA((count,))],
        input_output_aliases={1: 0} if extra else {},
        compiler_params=pltpu.CompilerParams(vmem_limit_bytes=VMEM),
        cost_estimate=cost(2e9, 1 << 23),
    )(both, *extra)


def rope_tables(seq_len, head_dim):
    half_dim = head_dim // 2
    inv_freq = ROPE_BASE ** (-jnp.arange(half_dim, dtype=F32) * (2.0 / head_dim))
    angles = jnp.arange(seq_len, dtype=F32)[:, None] * inv_freq[None, :]
    return jnp.cos(angles), jnp.sin(angles)


def solution(mesh):
    groups, members = mesh.devices.shape
    chips = members // CORES
    assert chips == CHIPS
    fine = Mesh(mesh.devices.reshape(groups, chips, CORES), ("dp", "x", "core"))
    tp = ("x", "core")

    def swap(value):
        return lax.ppermute(value, "core", [(0, 1), (1, 0)])

    def layers_body(hidden, lengths, w_query, w_key, w_value, w_out, w_gate, w_up, w_down, norm_attn, norm_mlp):
        core = lax.axis_index("core")
        layers = w_query.shape[0]
        _, seq, width = hidden.shape
        head = w_query.shape[-1]
        rows = seq // CHUNKS
        length = lax.dynamic_slice_in_dim(lengths, core, 1)
        cos_t, sin_t = rope_tables(seq, head)
        qkv_w = []
        for w in (w_query, w_key, w_value):
            own = w.reshape(layers, width, head)
            qkv_w += [own, swap(own)]
        ff_w = []
        for w in (w_gate, w_up, w_down):
            ff_w += [w, swap(w)]
        out_w = []
        for l in range(layers):
            mine = lax.all_gather(w_out[l].reshape(head, width), "x")
            out_w.append([mine, swap(mine)])
        x = [hidden] * CHUNKS
        k_cache, v_cache = [], []
        waiting = []
        ident = iter(range(1000))
        both = [None] * CHUNKS

        def carry(call, most):
            now = waiting[:most]
            del waiting[:most]
            made, results = call([make() for make, _ in now], next(ident))
            for (_, sink), result in zip(now, results):
                sink(result)
            return made

        def send_sum(i, parts, final):
            def landed(got):
                if final:
                    both[i] = lax.all_gather(got[0], tp).reshape(chips, CORES, *got[0].shape)
                else:
                    x[i] = lax.all_gather(got[0], "x", axis=0, tiled=True)

            waiting.append((lambda: Reduce(*parts), landed))

        for l in range(layers):
            final = l == layers - 1
            old = [[], [], [], []]
            o_all = [None] * CHUNKS
            for i in range(CHUNKS):
                made = carry(
                    lambda comms, n: front_call(l, i, length, norm_attn[l][None, :], cos_t, sin_t, x[i], qkv_w, old, rows, comms, n),
                    0 if l == 0 and i < 2 else 1,
                )
                old = [group + [k] for group, k in zip(old, made[:4])]
                o = made[4]
                waiting.append((lambda o=o: Gather(o), lambda got, i=i, o=o: o_all.__setitem__(i, [o, *got])))
            for i in range(CHUNKS):
                made = carry(
                    lambda comms, n: back_call(l, i, norm_mlp[l][None, :], x[i], o_all[i], out_w[l], ff_w, rows, comms, n),
                    2,
                )
                send_sum(i, made, final)
            for cache, own, theirs in ((k_cache, old[0], old[1]), (v_cache, old[2], old[3])):
                own = jnp.concatenate(own, axis=0)
                got = swap(jnp.concatenate(theirs, axis=0))
                cache.append(jnp.where(core == 0, jnp.stack([own, got]), jnp.stack([got, own]))[:, None])
        while waiting:
            carry(lambda comms, n: ([], idle_call(comms, n)), 2)
        h_out = None
        for i in range(CHUNKS):
            h_out = place_call(i, both[i], h_out, hidden.shape)
        return h_out, jnp.stack(k_cache), jnp.stack(v_cache)

    head_cols = P(None, None, tp, None)
    step = jax.shard_map(
        layers_body,
        mesh=fine,
        in_specs=(P("dp"), P("dp"), head_cols, head_cols, head_cols, P(None, tp, None, None), P(None, None, tp), P(None, None, tp), P(None, tp, None), P(), P()),
        out_specs=(P("dp"), P(None, "dp", tp), P(None, "dp", tp)),
        check_vma=False,
    )
    return lambda *args: step(*args)
```

```python
import functools

import jax
import jax.numpy as jnp
from jax import lax
from jax.experimental import pallas as pl
from jax.experimental.pallas import tpu as pltpu
from jax.sharding import Mesh
from jax.sharding import PartitionSpec as P


RMS_EPS = 1e-6
ROPE_BASE = 10000.0
CORES = 2
CHIPS = 4
CHUNKS = 4
ROW_TILE = 256
FF_TILE = 256
VMEM = 60 * 1024 * 1024
BF16 = jnp.bfloat16
F32 = jnp.float32
ANY = pl.BlockSpec(memory_space=pl.ANY)
SMEM = pl.BlockSpec(memory_space=pltpu.SMEM)
OFFSETS = (0, 3, 1, 2)
MESH = pl.DeviceIdType.MESH


def cost(flops, nbytes, exps=0):
    return pl.CostEstimate(flops=int(flops), bytes_accessed=int(nbytes), transcendentals=int(exps))


def norm_rows(x_f32, gain):
    mean_sq = jnp.mean(x_f32 * x_f32, axis=-1, keepdims=True)
    return (x_f32 * lax.rsqrt(mean_sq + RMS_EPS) * (1.0 + gain)).astype(BF16)


def struct(shape, dtype=BF16):
    return jax.ShapeDtypeStruct(shape, dtype)


def whole(shape):
    return pl.BlockSpec(shape, lambda *_: (0,) * len(shape))


def piece_rows(place, part):
    return pl.multiple_of(lax.rem(lax.axis_index("x") + OFFSETS[place], CHIPS) * part, part)


def to_right():
    return {"x": lax.rem(lax.axis_index("x") + 1, CHIPS)}


def to_left():
    return {"x": lax.rem(lax.axis_index("x") + CHIPS - 1, CHIPS)}


def remote(src, dst, send, recv, device):
    return pltpu.make_async_remote_copy(src_ref=src, dst_ref=dst, send_sem=send, recv_sem=recv, device_id=device, device_id_type=MESH)


class Gather:
    def __init__(self, block):
        self.inputs = [block]
        shape = struct(block.shape, block.dtype)
        self.out_shapes, self.out_specs = [shape] * 3, [ANY] * 3
        self.scratch = [pltpu.SemaphoreType.DMA((6,)), pltpu.SemaphoreType.DMA((6,))]

    def bind(self, inputs, outputs, scratch):
        own, (r, l, f), (send, recv) = inputs[0], outputs, scratch
        half = own.shape[0] // 2
        top, low = pl.ds(0, half), pl.ds(half, half)
        first = lambda: (
            remote(own.at[top], r.at[top], send.at[0], recv.at[0], to_right()),
            remote(own.at[low], l.at[low], send.at[1], recv.at[1], to_left()),
        )
        rest = lambda: (
            remote(own.at[low], r.at[low], send.at[4], recv.at[4], to_right()),
            remote(own.at[top], l.at[top], send.at[5], recv.at[5], to_left()),
        )
        second = lambda: (
            remote(r.at[top], f.at[top], send.at[2], recv.at[2], to_right()),
            remote(l.at[low], f.at[low], send.at[3], recv.at[3], to_left()),
        )

        def begin():
            for c in (*first(), *rest()):
                c.start()

        def onward():
            for a, b in zip(first(), second()):
                a.wait_recv()
                b.start()

        def finish():
            for c in first():
                c.wait_send()
            for c in (*rest(), *second()):
                c.wait()

        return {0: begin, 1: onward, 3: finish}


class Reduce:
    def __init__(self, base, left, right, far):
        self.inputs = [base, left, right, far]
        rows, width = base.shape
        self.out_shapes, self.out_specs = [struct((rows, width))], [whole((rows, width))]
        half, full = pltpu.VMEM((rows // 2, width), BF16), pltpu.VMEM((rows, width), BF16)
        self.scratch = [half, half, half, half, full, full, pltpu.VMEM((rows, width), F32)]
        self.scratch += [pltpu.SemaphoreType.DMA((6,)), pltpu.SemaphoreType.DMA((6,)), pltpu.SemaphoreType.DMA((3,))]

    def bind(self, inputs, outputs, scratch):
        base, left, right, far = inputs
        t_r, t_l, add_r, add_l, in_r, in_l, base_v, send, recv, load = scratch
        rows = base.shape[0]
        half = rows // 2
        top, low = pl.ds(0, half), pl.ds(half, half)
        first = lambda: (
            remote(far.at[top], t_r, send.at[0], recv.at[0], to_right()),
            remote(far.at[low], t_l, send.at[1], recv.at[1], to_left()),
        )
        direct = lambda: (
            remote(right.at[low], in_r.at[low], send.at[2], recv.at[2], to_right()),
            remote(left.at[top], in_l.at[top], send.at[3], recv.at[3], to_left()),
        )
        second = lambda: (
            remote(add_r, in_r.at[top], send.at[4], recv.at[4], to_right()),
            remote(add_l, in_l.at[low], send.at[5], recv.at[5], to_left()),
        )
        local = lambda: (
            pltpu.make_async_copy(right.at[top], add_r, load.at[0]),
            pltpu.make_async_copy(left.at[low], add_l, load.at[1]),
            pltpu.make_async_copy(base, base_v, load.at[2]),
        )

        def begin():
            for c in (*first(), *direct(), *local()):
                c.start()

        def onward():
            for c in local():
                c.wait()
            for c, add, t in zip(first(), (add_r, add_l), (t_r, t_l)):
                c.wait_recv()
                add[...] = (add[...].astype(F32) + t[...].astype(F32)).astype(BF16)
            for c in second():
                c.start()

        def finish():
            for c in first():
                c.wait_send()
            for c in (*direct(), *second()):
                c.wait()
            outputs[0][...] = (base_v[...] + in_r[...].astype(F32) + in_l[...].astype(F32)).astype(BF16)

        return {0: begin, 1: onward, 3: finish}


def stage(compute, inputs, in_specs, out_shapes, out_specs, scratch, comms, grid, cost_estimate, ident):
    sizes = [(len(c.inputs), len(c.out_shapes), len(c.scratch)) for c in comms]
    counts = [len(inputs), len(out_shapes), len(scratch)]
    all_in, all_specs = list(inputs), list(in_specs)
    all_shapes, all_outs, all_scratch = list(out_shapes), list(out_specs), list(scratch)
    for c in comms:
        all_in += c.inputs
        all_specs += [ANY] * len(c.inputs)
        all_shapes += c.out_shapes
        all_outs += c.out_specs
        all_scratch += c.scratch
    total_in, total_out = len(all_in), len(all_shapes)

    def kernel(*refs):
        groups = [list(refs[:total_in]), list(refs[total_in : total_in + total_out]), list(refs[total_in + total_out :])]
        mine = [g[:n] for g, n in zip(groups, counts)]
        rest = [g[n:] for g, n in zip(groups, counts)]
        acts = []
        for c, size in zip(comms, sizes):
            acts.append(c.bind(*[g[:n] for g, n in zip(rest, size)]))
            rest = [g[n:] for g, n in zip(rest, size)]

        def at(point):
            if point == 0 and comms:
                barrier = pltpu.get_barrier_semaphore()
                targets = [to_right(), to_left()]
                for t in targets:
                    pl.semaphore_signal(barrier, inc=1, device_id=t, device_id_type=MESH)
                pl.semaphore_wait(barrier, len(targets))
            for a in acts:
                if point in a:
                    a[point]()

        compute(*mine, at)

    extra = dict(collective_id=ident, has_side_effects=True) if comms else {}
    out = pl.pallas_call(
        kernel,
        grid=grid,
        out_shape=all_shapes,
        in_specs=all_specs,
        out_specs=all_outs,
        scratch_shapes=all_scratch,
        compiler_params=pltpu.CompilerParams(vmem_limit_bytes=VMEM, **extra),
        cost_estimate=cost_estimate,
    )(*all_in)
    made = list(out[: counts[1]])
    rest = list(out[counts[1] :])
    results = []
    for _, n, _ in sizes:
        results.append(rest[:n])
        rest = rest[n:]
    return made, results


def front_body(layer, chunk, from_hidden, inputs, outputs, scratch, at):
    at(0)
    refs = list(inputs)
    len_ref, gain_ref, cos_ref, sin_ref, x_ref = (refs.pop(0) for _ in range(5))
    w_refs = [refs.pop(0) for _ in range(6)]
    old = [[refs.pop(0) for _ in range(chunk)] for _ in range(4)]
    new, o_ref = outputs[:4], outputs[4]
    x_buf, normed, w_buf, q_buf, x_sem, w_sem = scratch
    rows, _ = x_buf.shape
    head = q_buf.shape[-1]
    half = head // 2
    x_copy = pltpu.make_async_copy(x_ref.at[lax.axis_index("core"), pl.ds(chunk * rows, rows)] if from_hidden else x_ref, x_buf, x_sem)
    x_copy.start()
    loads = [pltpu.make_async_copy(w_refs[n].at[layer], w_buf.at[n], w_sem.at[n]) for n in range(6)]
    for c in loads:
        c.start()
    x_copy.wait()
    tile = min(ROW_TILE, rows)
    for r in range(0, rows, tile):
        normed[pl.ds(r, tile)] = norm_rows(x_buf[pl.ds(r, tile)].astype(F32), gain_ref[...])

    def rope(y, r):
        low, high = y[:, :half], y[:, half:]
        c, s = cos_ref[pl.ds(r, tile)], sin_ref[pl.ds(r, tile)]
        return jnp.concatenate([low * c - high * s, high * c + low * s], axis=-1)

    for n in range(6):
        loads[n].wait()
        for r in range(0, rows, tile):
            y = jnp.dot(normed[pl.ds(r, tile)], w_buf[n], preferred_element_type=F32)
            if n < 2:
                q_buf[n, pl.ds(r, tile)] = (rope(y, r) * head**-0.5).astype(BF16)
            elif n < 4:
                new[n - 2][pl.ds(r, tile)] = rope(y, r).astype(BF16)
            else:
                new[n - 2][pl.ds(r, tile)] = y.astype(BF16)
    at(1)
    dims = (((1,), (1,)), ((), ()))
    length = len_ref[0]
    col = lax.broadcasted_iota(jnp.int32, (1, rows), 1)
    lower = lax.broadcasted_iota(jnp.int32, (tile, rows), 1) - lax.broadcasted_iota(jnp.int32, (tile, rows), 0)
    bias = [jnp.where(col < length - j * rows, 0.0, -1e30).astype(F32) for j in range(chunk + 1)]
    for h in range(2):
        keys = old[h] + [new[h]]
        values = old[2 + h] + [new[2 + h]]
        for r in range(0, rows, tile):
            query = q_buf[h, pl.ds(r, tile)]
            blocks = []
            for j in range(chunk + 1):
                scores = lax.dot_general(query, keys[j][...], dims, preferred_element_type=F32) + bias[j]
                if j == chunk:
                    scores = jnp.where(lower <= r, scores, -1e30)
                blocks.append(scores)
            top = functools.reduce(jnp.maximum, [jnp.max(b, axis=-1, keepdims=True) for b in blocks])
            blocks = [jnp.exp(b - top) for b in blocks]
            inv = 1.0 / functools.reduce(jnp.add, [jnp.sum(b, axis=-1, keepdims=True) for b in blocks])
            total = None
            for j in range(chunk + 1):
                prod = jnp.dot((blocks[j] * inv).astype(BF16), values[j][...], preferred_element_type=F32)
                total = prod if total is None else total + prod
            o_ref[pl.ds(r, tile), pl.ds(h * head, head)] = total.astype(BF16)
        if h == 0:
            at(2)
    at(3)


def front_call(layer, chunk, length, gain, cos_t, sin_t, x, weights, old, rows, comms, ident):
    width, head = weights[0].shape[1:]
    small = whole((rows, head))
    table = pl.BlockSpec((rows, head // 2), lambda *_: (chunk, 0))
    flops = 12 * rows * width * head + 8 * rows * rows * (chunk + 1) * head
    shapes, specs = [struct((rows, head))] * 4 + [struct((rows, 2 * head))], [small] * 4 + [whole((rows, 2 * head))]
    return stage(
        functools.partial(front_body, layer, chunk, x.ndim == 3),
        [length, gain, cos_t, sin_t, x, *weights, *[k for group in old for k in group]],
        [SMEM, whole((1, width)), table, table] + [ANY] * 7 + [small] * (4 * chunk),
        shapes,
        specs,
        [
            pltpu.VMEM((rows, width), BF16),
            pltpu.VMEM((rows, width), BF16),
            pltpu.VMEM((6, width, head), BF16),
            pltpu.VMEM((2, rows, head), BF16),
            pltpu.SemaphoreType.DMA,
            pltpu.SemaphoreType.DMA((6,)),
        ],
        comms,
        (1,),
        cost(flops, 12 * width * head + 4 * rows * width, 2 * rows * rows * (chunk + 1)),
        ident,
    )


def back_body(layer, chunk, from_hidden, inputs, outputs, scratch, at):
    gain_ref, x_ref = inputs[:2]
    o_refs, w_refs, ff, down_refs = inputs[2:6], inputs[6:8], inputs[8:12], inputs[12:]
    x_buf, o_buf, w_buf, normed, acc, act, down, x_sem, o_sem, w_sem, down_sem = scratch
    rows, _ = x_buf.shape
    inner = o_refs[0].shape[-1]
    head = inner // 2
    part = rows // CHIPS
    step = pl.program_id(0)
    tile = min(ROW_TILE, rows)
    cut_ff = ff[0].shape[-1]
    ff_rows = down.shape[0] // 2
    down_copies = [pltpu.make_async_copy(down_refs[n].at[layer], down.at[pl.ds(n * ff_rows, ff_rows)], down_sem.at[n]) for n in range(2)]

    @pl.when(step == 0)
    def _():
        src = x_ref.at[lax.axis_index("core"), pl.ds(chunk * rows, rows)] if from_hidden else x_ref
        x_copy = pltpu.make_async_copy(src, x_buf, x_sem)
        o_copies = [pltpu.make_async_copy(o_refs[n], o_buf.at[:, pl.ds(n * inner, inner)], o_sem.at[n]) for n in range(CHIPS)]
        w_copies = []
        for n in range(CHIPS):
            whose = lax.rem(lax.axis_index("x") + OFFSETS[n], CHIPS)
            for k in range(2):
                w_copies.append(
                    pltpu.make_async_copy(w_refs[k].at[whose], w_buf.at[pl.ds(n * inner + k * head, head)], w_sem.at[2 * n + k])
                )
        for n in range(CHIPS):
            o_copies[n].start()
            w_copies[2 * n].start()
            w_copies[2 * n + 1].start()
        x_copy.start()
        at(0)
        for c in down_copies:
            c.start()
        for group in range(2):
            for n in range(2 * group, 2 * group + 2):
                o_copies[n].wait()
                w_copies[2 * n].wait()
                w_copies[2 * n + 1].wait()
            if group == 1:
                x_copy.wait()
            cut = pl.ds(2 * group * inner, 2 * inner)
            prod = jnp.dot(o_buf[:, cut], w_buf[cut], preferred_element_type=F32)
            if group == 0:
                acc[...] = prod
            else:
                acc[...] += prod
        for r in range(0, rows, tile):
            mid = (x_buf[pl.ds(r, tile)].astype(F32) + acc[pl.ds(r, tile)]).astype(BF16)
            x_buf[pl.ds(r, tile)] = mid
            normed[pl.ds(r, tile)] = norm_rows(mid.astype(F32), gain_ref[...])

    @pl.when(step == 1)
    def _():
        at(1)

    for n in range(2):
        columns = pl.ds(pl.multiple_of(n * ff_rows + step * cut_ff, cut_ff), cut_ff)
        gate = jnp.dot(normed[...], ff[n][...], preferred_element_type=F32)
        up = jnp.dot(normed[...], ff[2 + n][...], preferred_element_type=F32)
        act[:, columns] = (jax.nn.gelu(gate, approximate=True) * up).astype(BF16)

    @pl.when(step == pl.num_programs(0) - 1)
    def _():
        for c in down_copies:
            c.wait()
        acc[...] = jnp.dot(act[...], down[...], preferred_element_type=F32)
        own = pl.ds(piece_rows(0, part), part)
        outputs[0][...] = x_buf[own].astype(F32) + acc[own]
        for place in range(1, CHIPS):
            outputs[place][...] = acc[pl.ds(piece_rows(place, part), part)].astype(BF16)
        at(3)


def back_call(layer, chunk, gain, x, o_list, w_list, ff_w, rows, comms, ident):
    head, width = w_list[0].shape[1:]
    ff = ff_w[0].shape[-1]
    tile = min(FF_TILE, ff)
    col = pl.BlockSpec((None, width, tile), lambda i: (layer, 0, i))
    part = rows // CHIPS
    return stage(
        functools.partial(back_body, layer, chunk, x.ndim == 3),
        [gain, x, *o_list, *w_list, *ff_w],
        [whole((1, width))] + [ANY] * 7 + [col] * 4 + [ANY] * 2,
        [struct((part, width), F32)] + [struct((part, width))] * 3,
        [whole((part, width))] * 4,
        [
            pltpu.VMEM((rows, width), BF16),
            pltpu.VMEM((rows, 8 * head), BF16),
            pltpu.VMEM((8 * head, width), BF16),
            pltpu.VMEM((rows, width), BF16),
            pltpu.VMEM((rows, width), F32),
            pltpu.VMEM((rows, 2 * ff), BF16),
            pltpu.VMEM((2 * ff, width), BF16),
            pltpu.SemaphoreType.DMA,
            pltpu.SemaphoreType.DMA((CHIPS,)),
            pltpu.SemaphoreType.DMA((8,)),
            pltpu.SemaphoreType.DMA((2,)),
        ],
        comms,
        (ff // tile,),
        cost(12 * rows * width * ff + 16 * rows * head * width, 12 * width * ff + 16 * head * width + 8 * rows * width, 2 * rows * ff),
        ident,
    )


def idle_body(inputs, outputs, scratch, at):
    for point in range(4):
        at(point)


def idle_call(comms, ident):
    return stage(idle_body, [], [], [], [], [], comms, (1,), cost(2e10, 1 << 22), ident)[1]


def place_kernel(chunk, both_ref, *refs):
    h_ref, buf, in_sem, out_sem = refs[-4:]
    part = both_ref.shape[2]
    spots = [(c, k) for c in range(CHIPS) for k in range(CORES)]
    loads = [pltpu.make_async_copy(both_ref.at[c, k], buf.at[n], in_sem.at[n]) for n, (c, k) in enumerate(spots)]
    saves = [
        pltpu.make_async_copy(buf.at[n], h_ref.at[k, pl.ds((chunk * CHIPS + c) * part, part)], out_sem.at[n])
        for n, (c, k) in enumerate(spots)
    ]
    for copy in loads:
        copy.start()
    for load, save in zip(loads, saves):
        load.wait()
        save.start()
    for copy in saves:
        copy.wait()


def place_call(chunk, both, before, shape):
    extra = [] if before is None else [before]
    count = CHIPS * CORES
    return pl.pallas_call(
        functools.partial(place_kernel, chunk),
        out_shape=struct(shape),
        in_specs=[ANY] * (1 + len(extra)),
        out_specs=ANY,
        scratch_shapes=[pltpu.VMEM((count, *both.shape[2:]), BF16), pltpu.SemaphoreType.DMA((count,)), pltpu.SemaphoreType.DMA((count,))],
        input_output_aliases={1: 0} if extra else {},
        compiler_params=pltpu.CompilerParams(vmem_limit_bytes=VMEM),
        cost_estimate=cost(2e9, 1 << 23),
    )(both, *extra)


def rope_tables(seq_len, head_dim):
    half_dim = head_dim // 2
    inv_freq = ROPE_BASE ** (-jnp.arange(half_dim, dtype=F32) * (2.0 / head_dim))
    angles = jnp.arange(seq_len, dtype=F32)[:, None] * inv_freq[None, :]
    return jnp.cos(angles), jnp.sin(angles)


def solution(mesh):
    groups, members = mesh.devices.shape
    chips = members // CORES
    assert chips == CHIPS
    fine = Mesh(mesh.devices.reshape(groups, chips, CORES), ("dp", "x", "core"))
    tp = ("x", "core")

    def swap(value):
        return lax.ppermute(value, "core", [(0, 1), (1, 0)])

    def layers_body(hidden, lengths, w_query, w_key, w_value, w_out, w_gate, w_up, w_down, norm_attn, norm_mlp):
        core = lax.axis_index("core")
        layers = w_query.shape[0]
        _, seq, width = hidden.shape
        head = w_query.shape[-1]
        rows = seq // CHUNKS
        length = lax.dynamic_slice_in_dim(lengths, core, 1)
        cos_t, sin_t = rope_tables(seq, head)
        qkv_w = []
        for w in (w_query, w_key, w_value):
            own = w.reshape(layers, width, head)
            qkv_w += [own, swap(own)]
        ff_w = []
        for w in (w_gate, w_up, w_down):
            ff_w += [w, swap(w)]
        out_w = []
        for l in range(layers):
            mine = lax.all_gather(w_out[l].reshape(head, width), "x")
            out_w.append([mine, swap(mine)])
        x = [hidden] * CHUNKS
        k_cache, v_cache = [], []
        waiting = []
        ident = iter(range(1000))
        both = [None] * CHUNKS

        def carry(call, most):
            now = waiting[:most]
            del waiting[:most]
            made, results = call([make() for make, _ in now], next(ident))
            for (_, sink), result in zip(now, results):
                sink(result)
            return made

        def send_sum(i, parts, final):
            def landed(got):
                if final:
                    both[i] = lax.all_gather(got[0], tp).reshape(chips, CORES, *got[0].shape)
                else:
                    x[i] = lax.all_gather(got[0], "x", axis=0, tiled=True)

            waiting.append((lambda: Reduce(*parts), landed))

        for l in range(layers):
            final = l == layers - 1
            old = [[], [], [], []]
            o_all = [None] * CHUNKS
            for i in range(CHUNKS):
                made = carry(
                    lambda comms, n: front_call(l, i, length, norm_attn[l][None, :], cos_t, sin_t, x[i], qkv_w, old, rows, comms, n),
                    0 if l == 0 and i < 2 else 1,
                )
                old = [group + [k] for group, k in zip(old, made[:4])]
                o = made[4]
                waiting.append((lambda o=o: Gather(o), lambda got, i=i, o=o: o_all.__setitem__(i, [o, *got])))
            for i in range(CHUNKS):
                made = carry(
                    lambda comms, n: back_call(l, i, norm_mlp[l][None, :], x[i], o_all[i], out_w[l], ff_w, rows, comms, n),
                    2,
                )
                send_sum(i, made, final)
            for cache, own, theirs in ((k_cache, old[0], old[1]), (v_cache, old[2], old[3])):
                own = jnp.concatenate(own, axis=0)
                got = swap(jnp.concatenate(theirs, axis=0))
                cache.append(jnp.where(core == 0, jnp.stack([own, got]), jnp.stack([got, own]))[:, None])
        while waiting:
            carry(lambda comms, n: ([], idle_call(comms, n)), 2)
        h_out = None
        for i in range(CHUNKS):
            h_out = place_call(i, both[i], h_out, hidden.shape)
        return h_out, jnp.stack(k_cache), jnp.stack(v_cache)

    head_cols = P(None, None, tp, None)
    step = jax.shard_map(
        layers_body,
        mesh=fine,
        in_specs=(P("dp"), P("dp"), head_cols, head_cols, head_cols, P(None, tp, None, None), P(None, None, tp), P(None, None, tp), P(None, tp, None), P(), P()),
        out_specs=(P("dp"), P(None, "dp", tp), P(None, "dp", tp)),
        check_vma=False,
    )
    return lambda *args: step(*args)
```
